32 devices in a mesh: group: 2 (over core), replica: 16 (over z, y, x).
Axes of the slice: x: 2, y: 2, z: 4, core: 2. Of those that a mesh axis runs over, the one named last changes fastest.
Arguments:
- tokens: bfloat16 [2, 2, 2048, 1088], P(None, 'group', 'replica'), may hold values from -6 to 6
- out_grad: bfloat16 [2, 2, 2048, 1088], P(None, 'group', 'replica'), may hold values from -6 to 6
- positions: int32 [2, 2, 2048], P(None, 'group', 'replica'), may hold values from 0 to 2047, each once within a row
- prefix: int32 [2, 2], P(None, 'group'), may hold values from 204 to 1024
- ln1_gain: bfloat16 [1088], P('group'), may hold values from 0.099609375 to 1.8984375
- ln1_bias: bfloat16 [1088], P('group'), may hold values from -1.75 to 1.75
- w_qkv: bfloat16 [1088, 3264], P('group'), may hold values from -0.1875 to 0.1875
- b_query: bfloat16 [1088], P('group'), may hold values from -1.75 to 1.75
- b_value: bfloat16 [1088], P('group'), may hold values from -0.1875 to 0.1875
- w_attn_out: bfloat16 [1088, 1088], P('group'), may hold values from -3 to 3
- b_attn_out: bfloat16 [1088], P('group'), may hold values from -1.75 to 1.75
- ln2_gain: bfloat16 [1088], P('group'), may hold values from 0.099609375 to 1.8984375
- ln2_bias: bfloat16 [1088], P('group'), may hold values from -1.75 to 1.75
- w_fc: bfloat16 [1088, 4352], P('group'), may hold values from -0.1875 to 0.1875
- b_fc: bfloat16 [4352], P('group'), may hold values from -1.75 to 1.75
- w_proj: bfloat16 [4352, 1088], P('group'), may hold values from -0.09375 to 0.09375
- b_proj: bfloat16 [1088], P('group'), may hold values from -1.75 to 1.75
Outputs:
- result: bfloat16 [2, 2, 2048, 1088], P(None, 'group', 'replica')
- tokens_grad: bfloat16 [2, 2, 2048, 1088], P(None, 'group', 'replica')
- ln1_gain_grad: float32 [1088], P('group')
- ln1_bias_grad: float32 [1088], P('group')
- w_qkv_grad: float32 [1088, 3264], P('group')
- b_query_grad: float32 [1088], P('group')
- b_value_grad: float32 [1088], P('group')
- w_attn_out_grad: float32 [1088, 1088], P('group')
- b_attn_out_grad: float32 [1088], P('group')
- ln2_gain_grad: float32 [1088], P('group')
- ln2_bias_grad: float32 [1088], P('group')
- w_fc_grad: float32 [1088, 4352], P('group')
- b_fc_grad: float32 [4352], P('group')
- w_proj_grad: float32 [4352, 1088], P('group')
- b_proj_grad: float32 [1088], P('group')
The draws below stay inside these ranges and needn't reach their ends.
Inputs may be any that keep to these rules, and one draw needn't show every extreme that they name: Each sequence's positions are a permutation of 0 to 2048 - 1 over its slots.
All inputs are finite; a program needn't handle non-finite values.
Results may differ from the reference program's by a relative error of at most 0.02.
Values may be sent and summed in bfloat16 or wider, within the bound.
A program may use at most 256 MiB of HBM per device.

```python
import jax
import jax.numpy as jnp
from jax import lax

D = 1088
FF = 4352
HEADS = 17
HEAD_DIM = 64
MICRO = 2
SEQ_MB = 2
LENGTH = 2048


def plant(array, key, smallest, largest):
    place = [jax.random.randint(jax.random.fold_in(key, axis), (), 0, length) for axis, length in enumerate(array.shape)]
    longest = array.shape.index(max(array.shape))
    beside = place[:longest] + [(place[longest] + 1) % array.shape[longest]] + place[longest + 1:]
    return array.at[tuple(place)].set(smallest).at[tuple(beside)].set(largest)


def steps_of(rng, dims, shards, smallest, top_value):
    loudness = 1.0
    for axis_at, parts in shards:
        steps = jax.random.uniform(jax.random.fold_in(jax.random.fold_in(rng, 6), axis_at), (parts,), jnp.float32, smallest / len(shards), top_value / len(shards))
        loudness = loudness * jnp.repeat(jnp.exp(steps), dims[axis_at] // parts).reshape((-1,) + (1,) * (len(dims) - 1 - axis_at))
    return loudness


def normal_values(own_key, shape, scale, bound, shards=(), kind=jnp.bfloat16):
    factor_of = steps_of(own_key, shape, shards, -0.22, 0.18) if shards else 1.0
    entries = jax.random.normal(own_key, shape, jnp.float32) * scale * factor_of
    return jnp.minimum(jnp.maximum(entries, -bound), bound).astype(kind)


def setup_inputs(seed: int = 0) -> dict:
    seeds = jax.random.split(jax.random.key(seed), 18)
    tokens = normal_values(seeds[0], (MICRO, SEQ_MB, LENGTH, D), 1.0, 6.0, ((1, 2), (2, 16)))
    out_grad = normal_values(seeds[1], (MICRO, SEQ_MB, LENGTH, D), 1.0, 6.0, ((1, 2), (2, 16)))
    positions = jax.vmap(lambda own: jax.random.permutation(own, LENGTH))(jax.random.split(seeds[2], MICRO * SEQ_MB)).reshape((MICRO, SEQ_MB, LENGTH)).astype(jnp.int32)
    prefix = plant(jax.random.randint(seeds[3], (MICRO, SEQ_MB), LENGTH // 10, LENGTH // 2 + 1), jax.random.fold_in(seeds[3], 1), LENGTH // 10, (LENGTH // 2 + 1) - 1).astype(jnp.int32)
    ln1_gain = jnp.clip(1.0 + 0.18 * jax.random.normal(seeds[4], (D,), jnp.float32), 0.099609375, 1.8984375).astype(jnp.bfloat16)
    ln1_bias = normal_values(seeds[5], (D,), 0.3, 1.75, ((0, 2),))
    w_qkv = normal_values(seeds[6], (D, 3 * D), D ** -0.5, 0.1875, ((0, 2),))
    b_query = normal_values(seeds[7], (D,), 0.3, 1.75, ((0, 2),))
    b_value = normal_values(seeds[8], (D,), 0.03, 0.1875, ((0, 2),))
    w_attn_out = normal_values(seeds[9], (D, D), (max(1, 8 * D // LENGTH)) ** -0.5, 3.0, ((0, 2),))
    b_attn_out = normal_values(seeds[10], (D,), 0.3, 1.75, ((0, 2),))
    ln2_gain = jnp.clip(1.0 + 0.18 * jax.random.normal(seeds[11], (D,), jnp.float32), 0.099609375, 1.8984375).astype(jnp.bfloat16)
    ln2_bias = normal_values(seeds[12], (D,), 0.3, 1.75, ((0, 2),))
    w_fc = normal_values(seeds[13], (D, FF), D ** -0.5, 0.1875, ((0, 2),))
    b_fc = normal_values(seeds[14], (FF,), 0.3, 1.75, ((0, 2),))
    w_proj = normal_values(seeds[15], (FF, D), FF ** -0.5, 0.09375, ((0, 2),))
    b_proj = normal_values(seeds[16], (D,), 0.3, 1.75, ((0, 2),))
    return {"tokens": tokens, "out_grad": out_grad, "positions": positions, "prefix": prefix, "ln1_gain": ln1_gain, "ln1_bias": ln1_bias, "w_qkv": w_qkv, "b_query": b_query, "b_value": b_value, "w_attn_out": w_attn_out, "b_attn_out": b_attn_out, "ln2_gain": ln2_gain, "ln2_bias": ln2_bias, "w_fc": w_fc, "b_fc": b_fc, "w_proj": w_proj, "b_proj": b_proj}


@jax.custom_vjp
def low(v):
    return lax.optimization_barrier(v.astype(jnp.bfloat16)).astype(jnp.float32)

@jax.custom_vjp
def low_back(v):
    return v

def low_keep(v):
    return (low(v), None)

def low_pass(kept, grad):
    return (grad,)

def back_keep(v):
    return (v, None)

def back_low(kept, grad):
    return (low(grad),)
low.defvjp(low_keep, low_pass)
low_back.defvjp(back_keep, back_low)

def norm_rows(values, gain, shift):
    center = values - lax.optimization_barrier(jnp.mean(values, -1, keepdims=True))
    spread = lax.optimization_barrier(jnp.mean(center * center, -1, keepdims=True))
    return center * lax.rsqrt(spread + 1e-05) * gain + shift

def matmul(left, right):
    return jnp.dot(left, right, preferred_element_type=jnp.float32, precision=lax.Precision.HIGHEST)

def attend(queries, keys, values, places, prefix_len):
    length = queries.shape[0]
    block = min(512, length)
    query_blocks = queries.reshape(length // block, block, HEADS, HEAD_DIM)
    place_blocks = places.reshape(length // block, block)
    scale = HEAD_DIM ** (-0.5)

    def one_block(blockargs):
        query_part, query_place = blockargs
        scores = jnp.einsum('qhe,khe->hqk', query_part, keys, precision=lax.Precision.HIGHEST) * scale
        scores = low_back(scores)
        allowed = (places[None, :] <= query_place[:, None]) | (places[None, :] < prefix_len)
        scores = jnp.where(allowed[None], scores, -1e+30)
        highest = lax.optimization_barrier(jnp.max(scores, -1, keepdims=True))
        expo = jnp.exp(scores - highest)
        probs = low(expo / lax.optimization_barrier(jnp.sum(expo, -1, keepdims=True)))
        return jnp.einsum('hqk,khe->qhe', probs, values, precision=lax.Precision.HIGHEST)
    outputs = lax.map(jax.checkpoint(one_block), (query_blocks, place_blocks))
    return outputs.reshape(length, HEADS * HEAD_DIM)

def layer(rows, params, places, prefix_len):
    ln1_gain, ln1_bias, w_qkv, b_query, b_value, w_attn_out, b_attn_out, ln2_gain, ln2_bias, w_fc, b_fc, w_proj, b_proj = params
    width = rows.shape[-1]
    first = low(norm_rows(rows, ln1_gain, ln1_bias))
    joined = matmul(first, w_qkv)
    queries = low(low_back(joined[:, :width] + b_query))
    keys = low(low_back(joined[:, width:2 * width]))
    values = low(low_back(joined[:, 2 * width:] + b_value))
    shape = (rows.shape[0], HEADS, HEAD_DIM)
    attended = attend(queries.reshape(shape), keys.reshape(shape), values.reshape(shape), places, prefix_len)
    attended = low(low_back(attended))
    middle = rows + low_back(matmul(attended, w_attn_out)) + b_attn_out
    second = low(norm_rows(middle, ln2_gain, ln2_bias))
    hidden_in = low_back(matmul(second, w_fc) + b_fc)
    hidden = low(jax.nn.gelu(hidden_in, approximate=True))
    return middle + low_back(matmul(hidden, w_proj)) + b_proj

def reference(tokens, out_grad, positions, prefix, ln1_gain, ln1_bias, w_qkv, b_query, b_value, w_attn_out, b_attn_out, ln2_gain, ln2_bias, w_fc, b_fc, w_proj, b_proj):
    count = MICRO * SEQ_MB
    inputs = tokens.astype(jnp.float32).reshape(count, LENGTH, D)
    params = tuple((item.astype(jnp.float32) for item in (ln1_gain, ln1_bias, w_qkv, b_query, b_value, w_attn_out, b_attn_out, ln2_gain, ln2_bias, w_fc, b_fc, w_proj, b_proj)))
    places = positions.reshape(count, LENGTH).astype(jnp.int32)
    prefixes = prefix.reshape(count).astype(jnp.int32)

    def whole(inputs, params):

        def one_sequence(blockargs):
            rows, place_row, prefix_len = blockargs
            return layer(rows, params, place_row, prefix_len)
        return lax.map(jax.checkpoint(one_sequence), (inputs, places, prefixes))
    outputs, pull = jax.vjp(whole, inputs, params)
    input_grad, param_grads = pull(out_grad.astype(jnp.float32).reshape(count, LENGTH, D))
    result = outputs.reshape(MICRO, SEQ_MB, LENGTH, D).astype(jnp.bfloat16)
    tokens_grad = input_grad.reshape(MICRO, SEQ_MB, LENGTH, D).astype(jnp.bfloat16)
    return (result, tokens_grad, param_grads[0], param_grads[1], param_grads[2], param_grads[3], param_grads[4], param_grads[5], param_grads[6], param_grads[7], param_grads[8], param_grads[9], param_grads[10], param_grads[11], param_grads[12])
```

```python
import functools

import jax
import jax.numpy as jnp
from jax import lax
from jax.experimental import pallas as pl
from jax.experimental.pallas import tpu as pltpu
from jax.sharding import PartitionSpec as P

HEADS = 17
HEAD_DIM = 64
MESH = pl.DeviceIdType.MESH


def for_sending(array):

    def short(part):
        return part.astype(jnp.bfloat16) if part.dtype == jnp.float32 else part

    return jax.tree.map(short, array)


def norm_rows(values, gain, shift):
    center = values - jnp.mean(values, -1, keepdims=True)
    spread = jnp.mean(center * center, -1, keepdims=True)
    return center * lax.rsqrt(spread + 1e-05) * gain + shift


def gelu_tanh(values):
    return jax.nn.gelu(values, approximate=True)


def inner_rows(left, right):
    return lax.dot_general(
        left, right, (((0,), (0,)), ((), ())), preferred_element_type=jnp.float32
    )


def times_transposed(left, right):
    return lax.dot_general(
        left, right, (((1,), (1,)), ((), ())), preferred_element_type=jnp.float32
    )


def masked_scores(queries, keys, query_place, key_place, prefix_len, scale):
    scores = jnp.einsum("qhe,khe->hqk", queries, keys, preferred_element_type=jnp.float32) * scale
    allowed = (key_place[None, :] <= query_place[:, None]) | (key_place[None, :] < prefix_len)
    return jnp.where(allowed[None], scores, -1e30)


def reduce_grads(terms):
    owned = jax.tree.map(
        lambda part: part.astype(jnp.float32),
        lax.psum_scatter(for_sending(terms), "group", scatter_dimension=0, tiled=True),
    )
    return jax.tree.map(
        lambda part: part.astype(jnp.float32), lax.psum(for_sending(owned), "replica")
    )


def per_device_gather(
    tokens,
    out_grad,
    positions,
    prefix,
    ln1_gain,
    ln1_bias,
    w_qkv,
    b_query,
    b_value,
    w_attn_out,
    b_attn_out,
    ln2_gain,
    ln2_bias,
    w_fc,
    b_fc,
    w_proj,
    b_proj,
):
    shards = (
        ln1_gain,
        ln1_bias,
        w_qkv,
        b_query,
        b_value,
        w_attn_out,
        b_attn_out,
        ln2_gain,
        ln2_bias,
        w_fc,
        b_fc,
        w_proj,
        b_proj,
    )
    micro = tokens.shape[0]
    rows_here = tokens.shape[2]
    width = tokens.shape[3]
    scale = HEAD_DIM ** (-0.5)
    head_shape = (rows_here, HEADS, HEAD_DIM)
    all_places = lax.all_gather(positions, "replica", axis=2, tiled=True)
    outputs_list = []
    grads_list = []
    kept = None
    owned = None
    for step in range(micro):
        full = (
            lax.all_gather(shards[0], "group", axis=0, tiled=True),
            lax.all_gather(shards[1], "group", axis=0, tiled=True),
            lax.all_gather(shards[2], "group", axis=0, tiled=True),
            lax.all_gather(shards[3], "group", axis=0, tiled=True),
            lax.all_gather(shards[4], "group", axis=0, tiled=True),
            lax.all_gather(shards[5], "group", axis=0, tiled=True),
            lax.all_gather(shards[6], "group", axis=0, tiled=True),
            lax.all_gather(shards[7], "group", axis=0, tiled=True),
            lax.all_gather(shards[8], "group", axis=0, tiled=True),
            lax.all_gather(shards[9], "group", axis=0, tiled=True),
            lax.all_gather(shards[10], "group", axis=0, tiled=True),
            lax.all_gather(shards[11], "group", axis=0, tiled=True),
            lax.all_gather(shards[12], "group", axis=0, tiled=True),
        )
        (
            gain_one,
            shift_one,
            mat_qkv,
            bias_query,
            bias_value,
            mat_out,
            bias_out,
            gain_two,
            shift_two,
            mat_fc,
            bias_fc,
            mat_proj,
            bias_proj,
        ) = full
        gain_one = gain_one.astype(jnp.float32)
        shift_one = shift_one.astype(jnp.float32)
        bias_query = bias_query.astype(jnp.float32)
        bias_value = bias_value.astype(jnp.float32)
        bias_out = bias_out.astype(jnp.float32)
        gain_two = gain_two.astype(jnp.float32)
        shift_two = shift_two.astype(jnp.float32)
        bias_fc = bias_fc.astype(jnp.float32)
        bias_proj = bias_proj.astype(jnp.float32)
        rows_in = tokens[step, 0].astype(jnp.float32)
        query_place = positions[step, 0]
        key_place = all_places[step, 0]
        prefix_len = prefix[step, 0]
        normed_one, norm_one_pull = jax.vjp(norm_rows, rows_in, gain_one, shift_one)
        first = normed_one.astype(jnp.bfloat16)
        joined = jnp.dot(first, mat_qkv, preferred_element_type=jnp.float32)
        queries = (joined[:, :width] + bias_query).astype(jnp.bfloat16)
        keys = joined[:, width : 2 * width].astype(jnp.bfloat16)
        values = (joined[:, 2 * width :] + bias_value).astype(jnp.bfloat16)
        key_all, value_all = (
            lax.all_gather(keys, "replica", axis=0, tiled=True),
            lax.all_gather(values, "replica", axis=0, tiled=True),
        )
        length = key_all.shape[0]
        block = min(512, length)
        nblocks = length // block
        query_heads = queries.reshape(head_shape)
        key_blocks = key_all.reshape(nblocks, block, HEADS, HEAD_DIM)
        value_blocks = value_all.reshape(nblocks, block, HEADS, HEAD_DIM)
        place_blocks = key_place.reshape(nblocks, block)

        def attend_step(carry, blockargs):
            highest, total, summed = carry
            key_part, value_part, place_part = blockargs
            scores = masked_scores(
                query_heads, key_part, query_place, place_part, prefix_len, scale
            )
            new_high = jnp.maximum(highest, jnp.max(scores, -1))
            factor = jnp.exp(highest - new_high)
            expo = jnp.exp(scores - new_high[..., None])
            total = total * factor + jnp.sum(expo, -1)
            summed = summed * jnp.transpose(factor)[..., None] + jnp.einsum(
                "hqk,khe->qhe",
                expo.astype(jnp.bfloat16),
                value_part,
                preferred_element_type=jnp.float32,
            )
            return ((new_high, total, summed), None)

        start_carry = (
            jnp.full((HEADS, rows_here), -1e30, jnp.float32),
            jnp.zeros((HEADS, rows_here), jnp.float32),
            jnp.zeros(head_shape, jnp.float32),
        )
        (highest, total, summed), _ = lax.scan(
            attend_step, start_carry, (key_blocks, value_blocks, place_blocks)
        )
        log_total = highest + jnp.log(total)
        attended_f = summed / jnp.transpose(total)[..., None]
        attended = attended_f.reshape(rows_here, width).astype(jnp.bfloat16)
        middle = rows_in + jnp.dot(attended, mat_out, preferred_element_type=jnp.float32) + bias_out
        normed_two, norm_two_pull = jax.vjp(norm_rows, middle, gain_two, shift_two)
        second = normed_two.astype(jnp.bfloat16)
        hidden_in = jnp.dot(second, mat_fc, preferred_element_type=jnp.float32) + bias_fc
        hidden_f, gelu_pull = jax.vjp(gelu_tanh, hidden_in)
        hidden = hidden_f.astype(jnp.bfloat16)
        output_rows = (
            middle + jnp.dot(hidden, mat_proj, preferred_element_type=jnp.float32) + bias_proj
        )
        outputs_list.append(output_rows.astype(jnp.bfloat16))
        grad_top = out_grad[step, 0].astype(jnp.float32)
        grad_low = out_grad[step, 0]
        grad_bias_proj = jnp.sum(grad_top, 0)
        grad_mat_proj = inner_rows(hidden, grad_low)
        grad_hidden = times_transposed(grad_low, mat_proj)
        (grad_hidden_in,) = gelu_pull(grad_hidden)
        grad_hidden_in = grad_hidden_in.astype(jnp.bfloat16)
        grad_bias_fc = jnp.sum(grad_hidden_in, 0, dtype=jnp.float32)
        grad_mat_fc = inner_rows(second, grad_hidden_in)
        grad_second = times_transposed(grad_hidden_in, mat_fc)
        grad_middle_norm, grad_gain_two, grad_shift_two = norm_two_pull(grad_second)
        grad_middle = grad_top + grad_middle_norm
        grad_bias_out = jnp.sum(grad_middle, 0)
        grad_branch = grad_middle.astype(jnp.bfloat16)
        grad_mat_out = inner_rows(attended, grad_branch)
        grad_attended = times_transposed(grad_branch, mat_out).astype(jnp.bfloat16)
        grad_heads = grad_attended.reshape(head_shape)
        delta = jnp.transpose(jnp.sum(grad_heads.astype(jnp.float32) * attended_f, -1))

        def score_grads(
            query_part, grad_part, key_part, value_part, qplace, kplace, lse_part, delta_part
        ):
            scores = masked_scores(query_part, key_part, qplace, kplace, prefix_len, scale)
            probs = jnp.exp(scores - lse_part[..., None])
            grad_probs = jnp.einsum(
                "qhe,khe->hqk", grad_part, value_part, preferred_element_type=jnp.float32
            )
            grad_scores = (probs * (grad_probs - delta_part[..., None])).astype(jnp.bfloat16)
            return (probs.astype(jnp.bfloat16), grad_scores)

        def grad_step(summed, blockargs):
            key_part, value_part, place_part = blockargs
            probs, grad_scores = score_grads(
                query_heads,
                grad_heads,
                key_part,
                value_part,
                query_place,
                place_part,
                log_total,
                delta,
            )
            summed = summed + jnp.einsum(
                "hqk,khe->qhe", grad_scores, key_part, preferred_element_type=jnp.float32
            )
            key_grad = jnp.einsum(
                "hqk,qhe->khe", grad_scores, query_heads, preferred_element_type=jnp.float32
            )
            value_grad = jnp.einsum(
                "hqk,qhe->khe", probs, grad_heads, preferred_element_type=jnp.float32
            )
            return (summed, (key_grad, value_grad))

        grad_query, (key_grads, value_grads) = lax.scan(
            grad_step, jnp.zeros(head_shape, jnp.float32), (key_blocks, value_blocks, place_blocks)
        )
        grad_key, grad_value = (
            lax.psum_scatter(
                key_grads.reshape(length, width).astype(jnp.bfloat16),
                "replica",
                scatter_dimension=0,
                tiled=True,
            ).astype(jnp.float32),
            lax.psum_scatter(
                value_grads.reshape(length, width).astype(jnp.bfloat16),
                "replica",
                scatter_dimension=0,
                tiled=True,
            ).astype(jnp.float32),
        )
        grad_query = (grad_query.reshape(rows_here, width) * scale).astype(jnp.bfloat16)
        grad_key = (grad_key * scale).astype(jnp.bfloat16)
        grad_value = grad_value.astype(jnp.bfloat16)
        grad_bias_query = jnp.sum(grad_query, 0, dtype=jnp.float32)
        grad_bias_value = jnp.sum(grad_value, 0, dtype=jnp.float32)
        grad_joined = jnp.concatenate([grad_query, grad_key, grad_value], 1)
        grad_mat_qkv = inner_rows(first, grad_joined)
        grad_first = times_transposed(grad_joined, mat_qkv)
        grad_rows_norm, grad_gain_one, grad_shift_one = norm_one_pull(grad_first)
        grads_list.append((grad_middle + grad_rows_norm).astype(jnp.bfloat16))
        terms = (
            grad_gain_one,
            grad_shift_one,
            grad_mat_qkv,
            grad_bias_query,
            grad_bias_value,
            grad_mat_out,
            grad_bias_out,
            grad_gain_two,
            grad_shift_two,
            grad_mat_fc,
            grad_bias_fc,
            grad_mat_proj,
            grad_bias_proj,
        )
        kept = (
            terms
            if kept is None
            else tuple((first_term + second_term for first_term, second_term in zip(kept, terms)))
        )
    owned = reduce_grads(kept)
    result = jnp.stack(outputs_list).reshape(micro, 1, rows_here, width)
    tokens_grad = jnp.stack(grads_list).reshape(micro, 1, rows_here, width)
    return (result, tokens_grad) + tuple(owned)


def contract(left, right, left_dim, right_dim):
    return lax.dot_general(
        left, right, (((left_dim,), (right_dim,)), ((), ())), preferred_element_type=jnp.float32
    )


def greet(peers, here, group_too):
    barrier = pltpu.get_barrier_semaphore()

    def one(step, carry):
        peer = lax.rem(here + step, peers)
        pl.semaphore_signal(barrier, inc=1, device_id={"replica": peer}, device_id_type=MESH)
        return carry

    lax.fori_loop(1, peers, one, 0)
    if group_too:
        other = 1 - lax.axis_index("group")
        pl.semaphore_signal(barrier, inc=1, device_id={"group": other}, device_id_type=MESH)
    pl.semaphore_wait(barrier, peers - 1 + (1 if group_too else 0))


def exchange_body(direction, with_places, nweights, *refs):
    refs = list(refs)
    chunk, last = refs.pop(0), refs.pop(0)
    places = refs.pop(0) if with_places else None
    weights = [refs.pop(0) for _ in range(nweights)]
    chunk_out, last_out = refs.pop(0), refs.pop(0)
    places_out = refs.pop(0) if with_places else None
    weights_out = [refs.pop(0) for _ in range(nweights)]
    send, recv, last_send, last_recv, own = (refs.pop(0) for _ in range(5))
    if with_places:
        place_send, place_recv = refs.pop(0), refs.pop(0)
    if nweights:
        weight_send, weight_recv, weight_own = (refs.pop(0) for _ in range(3))
        bounce = [refs.pop(0) for _ in range(nweights)]
    peers = chunk.shape[0]
    here = lax.axis_index("replica")
    group = lax.axis_index("group")
    greet(peers, here, nweights > 0)
    loads, copies = [], []
    for i in range(nweights):
        copy = pltpu.make_async_remote_copy(
            weights[i],
            weights_out[i].at[group],
            weight_send.at[i],
            weight_recv.at[i],
            device_id={"group": 1 - group},
            device_id_type=MESH,
        )
        copy.start()
        copies.append(copy)
        load = pltpu.make_async_copy(weights[i], bounce[i], weight_own.at[i])
        load.start()
        loads.append(load)
    for slot in range(2):
        half = peers // 2
        target = lax.rem(here + direction + peers, half) + half * slot
        copy = pltpu.make_async_remote_copy(
            last.at[slot],
            last_out.at[here // half],
            last_send.at[slot],
            last_recv.at[here // half],
            device_id={"replica": target},
            device_id_type=MESH,
        )
        copy.start()
        copies.append(
            (
                copy,
                pltpu.make_async_remote_copy(
                    last.at[slot],
                    last_out.at[slot],
                    last_send.at[slot],
                    last_recv.at[slot],
                    device_id={"replica": target},
                    device_id_type=MESH,
                ),
            )
        )
    for step in range(1, peers):
        peer = lax.rem(here + step, peers)
        copy = pltpu.make_async_remote_copy(
            chunk.at[peer],
            chunk_out.at[here],
            send.at[step],
            recv.at[step],
            device_id={"replica": peer},
            device_id_type=MESH,
        )
        copy.start()
        copies.append(copy)
        if with_places:
            copy = pltpu.make_async_remote_copy(
                places,
                places_out.at[here],
                place_send.at[step],
                place_recv.at[step],
                device_id={"replica": peer},
                device_id_type=MESH,
            )
            copy.start()
            copies.append(copy)
    owns = [pltpu.make_async_copy(chunk.at[here], chunk_out.at[here], own.at[0])]
    if with_places:
        owns.append(pltpu.make_async_copy(places, places_out.at[here], own.at[1]))
    for copy in owns:
        copy.start()
    stores = []
    for i, load in enumerate(loads):
        load.wait()
        store = pltpu.make_async_copy(bounce[i], weights_out[i].at[group], weight_own.at[i])
        store.start()
        stores.append(store)
    for copy in stores + owns:
        copy.wait()
    for copy in copies:
        if isinstance(copy, tuple):
            copy[0].wait_send()
            copy[1].wait_recv()
        else:
            copy.wait()


def exchange(ident, direction, chunk, last, places=None, weights=()):
    peers = chunk.shape[0]
    any_spec = pl.BlockSpec(memory_space=pl.ANY)
    with_places = places is not None
    args = [chunk, last] + ([places] if with_places else []) + list(weights)
    shapes = [(chunk.shape, chunk.dtype), (last.shape, last.dtype)]
    if with_places:
        shapes.append(((peers,) + places.shape, places.dtype))
    shapes += [((2,) + weight.shape, weight.dtype) for weight in weights]
    dma = pltpu.SemaphoreType.DMA
    scratch = [dma((peers,)), dma((peers,)), dma((2,)), dma((2,)), dma((2,))]
    if with_places:
        scratch += [dma((peers,)), dma((peers,))]
    if weights:
        count = len(weights)
        scratch += [dma((count,)), dma((count,)), dma((count,))]
        scratch += [pltpu.VMEM(weight.shape, weight.dtype) for weight in weights]
    return pl.pallas_call(
        functools.partial(exchange_body, direction, with_places, len(weights)),
        out_shape=[jax.ShapeDtypeStruct(*shape) for shape in shapes],
        in_specs=[any_spec] * len(args),
        out_specs=[any_spec] * len(shapes),
        scratch_shapes=scratch,
        compiler_params=pltpu.CompilerParams(collective_id=ident, has_side_effects=True),
        name=f"exchange{ident}",
    )(*args)


def share_body(count, *refs):
    sources, results = refs[:count], refs[count : 2 * count]
    send, recv, own = refs[2 * count : 2 * count + 3]
    bounce = refs[2 * count + 3 :]
    group = lax.axis_index("group")
    barrier = pltpu.get_barrier_semaphore()
    pl.semaphore_signal(barrier, inc=1, device_id={"group": 1 - group}, device_id_type=MESH)
    pl.semaphore_wait(barrier, 1)
    copies, loads, stores = [], [], []
    for i in range(count):
        copy = pltpu.make_async_remote_copy(
            sources[i],
            results[i].at[group],
            send.at[i],
            recv.at[i],
            device_id={"group": 1 - group},
            device_id_type=MESH,
        )
        copy.start()
        copies.append(copy)
        load = pltpu.make_async_copy(sources[i], bounce[i], own.at[i])
        load.start()
        loads.append(load)
    for i in range(count):
        loads[i].wait()
        store = pltpu.make_async_copy(bounce[i], results[i].at[group], own.at[i])
        store.start()
        stores.append(store)
    for copy in stores + copies:
        copy.wait()


def share(ident, *arrays):
    count = len(arrays)
    any_spec = pl.BlockSpec(memory_space=pl.ANY)
    dma = pltpu.SemaphoreType.DMA
    return pl.pallas_call(
        functools.partial(share_body, count),
        out_shape=[jax.ShapeDtypeStruct((2,) + a.shape, a.dtype) for a in arrays],
        in_specs=[any_spec] * count,
        out_specs=[any_spec] * count,
        scratch_shapes=[dma((count,)), dma((count,)), dma((count,))]
        + [pltpu.VMEM(a.shape, a.dtype) for a in arrays],
        compiler_params=pltpu.CompilerParams(collective_id=ident, has_side_effects=True),
        name=f"share{ident}",
    )(*arrays)


BLOCK = 256


def unpack_units(got, last, rows_at, query_out):
    peers = got.shape[0]
    half = BLOCK // 128
    for m in range(2):
        for s in range(peers):
            query_out[m * (peers // half) + s // half, :, (s % half) * 128 : (s % half + 1) * 128] = got[
                s, rows_at : rows_at + 64, m * 128 : (m + 1) * 128
            ]
    extra = 2 * (peers // half)
    for j in range(2):
        query_out[extra, :, j * 128 : (j + 1) * 128] = last[j]


def unit_source(got, u, s, first):
    if u < 2:
        return got[s, first : first + 64, u * 128 : (u + 1) * 128]
    at = 0 if first == 64 else 128
    return got[s, 192:256, at : at + 128]


def attend_body(got, last, limit, places, sent, last_sent, out_f, lse, keys, values, queries, outs):
    peers = got.shape[0]
    nblocks = queries.shape[0]
    per_unit = (nblocks - 1) // 2
    unpack_units(got, last, 0, queries)
    for u in range(3):
        for s in range(peers):
            span = slice(s * 128, (s + 1) * 128)
            keys[u, span, :] = unit_source(got, u, s, 64).T
            values[u, :, span] = unit_source(got, u, s, 128)

    def block(b, carry):
        u = b // per_unit
        scores = jnp.dot(keys[u], queries[b], preferred_element_type=jnp.float32)
        place = places[u]
        place = jnp.concatenate([place, place], axis=1)
        scores = jnp.where(place < limit[b], scores, -1e30)
        high = jnp.max(scores, axis=0, keepdims=True)
        expo = jnp.exp(scores - high)
        total = jnp.sum(expo, axis=0, keepdims=True)
        summed = jnp.dot(values[u], expo.astype(jnp.bfloat16), preferred_element_type=jnp.float32)
        result = summed / total
        out_f[b] = result
        outs[b] = result.astype(jnp.bfloat16)
        lse[b] = high + jnp.log(total)
        return carry

    lax.fori_loop(0, nblocks, block, 0)
    half = BLOCK // 128
    for m in range(2):
        for s in range(peers):
            sent[s, :, m * 128 : (m + 1) * 128] = outs[
                m * per_unit + s // half, :, (s % half) * 128 : (s % half + 1) * 128
            ]
    for j in range(2):
        last_sent[j] = outs[nblocks - 1, :, j * 128 : (j + 1) * 128]


def attend(got, last, limit, places):
    peers = got.shape[0]
    nblocks = limit.shape[0]
    length = places.shape[1]
    bf, f32 = jnp.bfloat16, jnp.float32
    return pl.pallas_call(
        attend_body,
        out_shape=[
            jax.ShapeDtypeStruct((peers, 64, 256), bf),
            jax.ShapeDtypeStruct((2, 64, 128), bf),
            jax.ShapeDtypeStruct((nblocks, 64, BLOCK), f32),
            jax.ShapeDtypeStruct((nblocks, 1, BLOCK), f32),
        ],
        scratch_shapes=[
            pltpu.VMEM((3, length, 64), bf),
            pltpu.VMEM((3, 64, length), bf),
            pltpu.VMEM((nblocks, 64, BLOCK), bf),
            pltpu.VMEM((nblocks, 64, BLOCK), bf),
        ],
        compiler_params=pltpu.CompilerParams(vmem_limit_bytes=56 << 20),
        name="attend",
    )(got, last, limit, places)


def attend_grad_body(
    got,
    last,
    limit,
    places,
    out_f,
    lse,
    grad_got,
    grad_last,
    sent,
    last_sent,
    keys,
    keys_t,
    values,
    queries,
    grads,
    queries_n,
    grads_n,
    dqs,
    dk,
    dv,
):
    peers = got.shape[0]
    nblocks = queries.shape[0]
    per_unit = (nblocks - 1) // 2
    unpack_units(got, last, 0, queries)
    unpack_units(grad_got, grad_last, 0, grads)
    for u in range(3):
        for s in range(peers):
            span = slice(s * 128, (s + 1) * 128)
            part = unit_source(got, u, s, 64)
            keys[u, span, :] = part.T
            keys_t[u, :, span] = part
            values[u, span, :] = unit_source(got, u, s, 128).T
    for b in range(nblocks):
        queries_n[b] = queries[b].T
        grads_n[b] = grads[b].T
    dk[...] = jnp.zeros_like(dk)
    dv[...] = jnp.zeros_like(dv)

    def block(b, carry):
        u = b // per_unit
        grad = grads[b]
        delta = jnp.sum(grad.astype(jnp.float32) * out_f[b], axis=0, keepdims=True)
        scores = jnp.dot(keys[u], queries[b], preferred_element_type=jnp.float32)
        place = places[u]
        place = jnp.concatenate([place, place], axis=1)
        scores = jnp.where(place < limit[b], scores, -1e30)
        probs = jnp.exp(scores - lse[b])
        grad_probs = jnp.dot(values[u], grad, preferred_element_type=jnp.float32)
        grad_scores = (probs * (grad_probs - delta)).astype(jnp.bfloat16)
        dqs[b] = jnp.dot(keys_t[u], grad_scores, preferred_element_type=jnp.float32)
        dk[u] += jnp.dot(grad_scores, queries_n[b], preferred_element_type=jnp.float32)
        dv[u] += jnp.dot(probs.astype(jnp.bfloat16), grads_n[b], preferred_element_type=jnp.float32)
        return carry

    lax.fori_loop(0, nblocks, block, 0)
    half = BLOCK // 128
    scale = HEAD_DIM ** (-0.5)
    for m in range(2):
        for s in range(peers):
            at = slice(m * 128, (m + 1) * 128)
            span = slice(s * 128, (s + 1) * 128)
            dq = dqs[m * per_unit + s // half, :, (s % half) * 128 : (s % half + 1) * 128]
            sent[s, 0:64, at] = (dq * scale).astype(jnp.bfloat16)
            sent[s, 64:128, at] = dk[m, span, :].T.astype(jnp.bfloat16)
            sent[s, 128:192, at] = dv[m, span, :].T.astype(jnp.bfloat16)
    for s in range(peers):
        span = slice(s * 128, (s + 1) * 128)
        sent[s, 192:256, 0:128] = dk[2, span, :].T.astype(jnp.bfloat16)
        sent[s, 192:256, 128:256] = dv[2, span, :].T.astype(jnp.bfloat16)
    for j in range(2):
        last_sent[j] = (dqs[nblocks - 1, :, j * 128 : (j + 1) * 128] * scale).astype(jnp.bfloat16)


def attend_grad(got, last, limit, places, out_f, lse, grad_got, grad_last):
    peers = got.shape[0]
    nblocks = limit.shape[0]
    length = places.shape[1]
    bf, f32 = jnp.bfloat16, jnp.float32
    return pl.pallas_call(
        attend_grad_body,
        out_shape=[
            jax.ShapeDtypeStruct((peers, 256, 256), bf),
            jax.ShapeDtypeStruct((2, 64, 128), bf),
        ],
        scratch_shapes=[
            pltpu.VMEM((3, length, 64), bf),
            pltpu.VMEM((3, 64, length), bf),
            pltpu.VMEM((3, length, 64), bf),
            pltpu.VMEM((nblocks, 64, BLOCK), bf),
            pltpu.VMEM((nblocks, 64, BLOCK), bf),
            pltpu.VMEM((nblocks, BLOCK, 64), bf),
            pltpu.VMEM((nblocks, BLOCK, 64), bf),
            pltpu.VMEM((nblocks, 64, BLOCK), f32),
            pltpu.VMEM((3, length, 64), f32),
            pltpu.VMEM((3, length, 64), f32),
        ],
        compiler_params=pltpu.CompilerParams(vmem_limit_bytes=60 << 20),
        name="attend_grad",
    )(got, last, limit, places, out_f, lse, grad_got, grad_last)


def split_last(array):
    return jnp.stack([array[:, :128], array[:, 128:]])


def per_device_heads(
    tokens,
    out_grad,
    positions,
    prefix,
    ln1_gain,
    ln1_bias,
    w_qkv,
    b_query,
    b_value,
    w_attn_out,
    b_attn_out,
    ln2_gain,
    ln2_bias,
    w_fc,
    b_fc,
    w_proj,
    b_proj,
):
    bf, f32 = jnp.bfloat16, jnp.float32
    micro, _, rows_here, width = tokens.shape
    peers = lax.axis_size("replica")
    hidden_width = 2 * b_fc.shape[0]
    half = peers // 2
    count = micro * rows_here
    here = lax.axis_index("replica")
    scale = HEAD_DIM ** (-0.5)
    split = (peers * HEAD_DIM, width)

    small = jnp.concatenate(
        [ln1_gain, ln1_bias, b_query, b_value, b_attn_out, ln2_gain, ln2_bias, b_proj, b_fc]
    ).reshape(1, -1)
    mat_qkv, vectors = share(1, w_qkv, small)
    mat_qkv = mat_qkv.reshape(width, 3 * width)
    vectors = vectors[:, 0].astype(f32)
    part = width // 2
    gain_one, shift_one, bias_query, bias_value, bias_out, gain_two, shift_two, bias_proj = (
        vectors[:, i * part : (i + 1) * part].reshape(width) for i in range(8)
    )
    bias_fc = vectors[:, 8 * part :].reshape(hidden_width)

    rows_in = tokens.reshape(count, width).astype(f32)
    normed_one, norm_one_pull = jax.vjp(norm_rows, rows_in, gain_one, shift_one)
    first = normed_one.astype(bf)
    joined = contract(mat_qkv, first, 0, 1)
    bias_all = jnp.concatenate([bias_query, jnp.zeros_like(bias_query), bias_value])
    joined = joined + bias_all[:, None]
    queries = ((joined[:width]).astype(bf).astype(f32) * scale).astype(bf)
    keys = joined[width : 2 * width].astype(bf)
    values = joined[2 * width :].astype(bf)
    cut = split[0]
    main = [part_[:cut].reshape(peers, HEAD_DIM, count) for part_ in (queries, keys, values)]
    key_last, value_last = keys[cut:], values[cut:]
    tails = jnp.stack(
        [
            jnp.concatenate(
                [key_last[:, m * 128 : (m + 1) * 128], value_last[:, m * 128 : (m + 1) * 128]], 1
            )
            for m in range(2)
        ]
    )
    tails = jnp.repeat(tails, half, axis=0)
    chunk = jnp.concatenate(main + [tails], axis=1)
    got, got_last, all_places, mat_out, mat_fc, mat_proj = exchange(
        2,
        1,
        chunk,
        split_last(queries[cut:]),
        positions.reshape(micro, rows_here),
        (w_attn_out, w_fc, w_proj),
    )
    mat_out = mat_out.reshape(width, width)
    mat_fc = mat_fc.reshape(width, hidden_width)
    mat_proj = mat_proj.reshape(hidden_width, width)

    place_rows = jnp.transpose(all_places, (1, 0, 2)).reshape(micro, peers * rows_here)
    limits = jnp.maximum(place_rows + 1, prefix.reshape(micro, 1))
    mine = here // half
    at = lax.rem(here - 1 + peers, half)
    own_limits = lax.dynamic_index_in_dim(limits, mine, 0, False).reshape(peers, rows_here)
    own_limits = jnp.concatenate(
        [
            lax.dynamic_index_in_dim(own_limits, at, 0, True),
            lax.dynamic_index_in_dim(own_limits, at + half, 0, True),
        ],
        1,
    )
    limit = jnp.concatenate([limits.reshape(-1, BLOCK), own_limits], 0)[:, None, :]
    unit_places = jnp.concatenate(
        [place_rows, lax.dynamic_index_in_dim(place_rows, mine, 0, True)], 0
    )
    unit_places = jnp.broadcast_to(unit_places[:, :, None], unit_places.shape + (128,))

    sent, sent_last, out_f, lse = attend(got, got_last, limit, unit_places)
    heads_out, heads_last = exchange(3, -1, sent, sent_last)
    attended = jnp.concatenate(
        [heads_out.reshape(cut, count), jnp.concatenate([heads_last[0], heads_last[1]], 1)], 0
    )

    middle = rows_in + contract(attended, mat_out, 0, 0) + bias_out
    normed_two, norm_two_pull = jax.vjp(norm_rows, middle, gain_two, shift_two)
    second = normed_two.astype(bf)
    hidden_in = jnp.dot(second, mat_fc, preferred_element_type=f32) + bias_fc
    hidden_f, gelu_pull = jax.vjp(gelu_tanh, hidden_in)
    hidden = hidden_f.astype(bf)
    output_rows = middle + jnp.dot(hidden, mat_proj, preferred_element_type=f32) + bias_proj
    result = output_rows.astype(bf).reshape(micro, 1, rows_here, width)

    grad_low = out_grad.reshape(count, width)
    grad_top = grad_low.astype(f32)
    grad_bias_proj = jnp.sum(grad_top, 0)
    grad_mat_proj = contract(hidden, grad_low, 0, 0)
    (grad_hidden_in,) = gelu_pull(times_transposed(grad_low, mat_proj))
    grad_hidden_in = grad_hidden_in.astype(bf)
    grad_bias_fc = jnp.sum(grad_hidden_in, 0, dtype=f32)
    grad_mat_fc = contract(second, grad_hidden_in, 0, 0)
    grad_second = times_transposed(grad_hidden_in, mat_fc)
    grad_middle_norm, grad_gain_two, grad_shift_two = norm_two_pull(grad_second)
    grad_middle = grad_top + grad_middle_norm
    grad_bias_out = jnp.sum(grad_middle, 0)
    grad_branch = grad_middle.astype(bf)
    grad_mat_out = contract(attended, grad_branch, 1, 0)
    grad_attended = contract(mat_out, grad_branch, 1, 1).astype(bf)

    grad_got, grad_got_last = exchange(
        4, 1, grad_attended[:cut].reshape(peers, HEAD_DIM, count), split_last(grad_attended[cut:])
    )
    grad_sent, grad_sent_last = attend_grad(
        got, got_last, limit, unit_places, out_f, lse, grad_got, grad_got_last
    )
    back, back_last = exchange(5, -1, grad_sent, grad_sent_last)
    last_parts = back[:, 192:256, :].astype(f32).reshape(2, half, HEAD_DIM, 256)
    last_sums = jnp.sum(last_parts, 1).astype(bf)
    grad_query = jnp.concatenate(
        [back[:, 0:64].reshape(cut, count), jnp.concatenate([back_last[0], back_last[1]], 1)], 0
    )
    grad_key = jnp.concatenate(
        [
            back[:, 64:128].reshape(cut, count),
            jnp.concatenate([last_sums[0, :, :128], last_sums[1, :, :128]], 1),
        ],
        0,
    )
    grad_value = jnp.concatenate(
        [
            back[:, 128:192].reshape(cut, count),
            jnp.concatenate([last_sums[0, :, 128:], last_sums[1, :, 128:]], 1),
        ],
        0,
    )
    grad_bias_query = jnp.sum(grad_query, 1, dtype=f32)
    grad_bias_value = jnp.sum(grad_value, 1, dtype=f32)
    grad_joined = jnp.concatenate([grad_query, grad_key, grad_value], 0)
    grad_mat_qkv = contract(first, grad_joined, 0, 1)
    grad_first = contract(grad_joined, mat_qkv, 0, 1)
    grad_rows_norm, grad_gain_one, grad_shift_one = norm_one_pull(grad_first)
    tokens_grad = (grad_middle + grad_rows_norm).astype(bf).reshape(micro, 1, rows_here, width)

    matrices = reduce_grads((grad_mat_qkv, grad_mat_out, grad_mat_fc, grad_mat_proj))
    small_grads = jnp.concatenate(
        [
            item.reshape(2, -1)
            for item in (
                grad_gain_one,
                grad_shift_one,
                grad_bias_query,
                grad_bias_value,
                grad_bias_out,
                grad_gain_two,
                grad_shift_two,
                grad_bias_proj,
                grad_bias_fc,
            )
        ],
        1,
    )
    small_grads = lax.psum(small_grads, ("group", "replica"))
    small_own = lax.dynamic_index_in_dim(small_grads, lax.axis_index("group"), 0, False)
    vec = [small_own[i * part : (i + 1) * part] for i in range(8)] + [small_own[8 * part :]]
    return (
        result,
        tokens_grad,
        vec[0],
        vec[1],
        matrices[0],
        vec[2],
        vec[3],
        matrices[1],
        vec[4],
        vec[5],
        vec[6],
        matrices[2],
        vec[8],
        matrices[3],
        vec[7],
    )


def specs():
    wide = P(None, "group", "replica", None)
    row, mat = P("group"), P("group", None)
    in_specs = (wide, wide, P(None, "group", "replica"), P(None, "group"))
    in_specs += (row, row, mat, row, row, mat, row, row, row, mat, row, mat, row)
    out_specs = (wide, wide, row, row, mat, row, row, mat, row, row, row, mat, row, mat, row)
    return in_specs, out_specs


def solution(mesh):
    by_heads = mesh.shape["replica"] == HEADS - 1 and mesh.shape["group"] == 2
    in_specs, out_specs = specs()
    return jax.shard_map(
        per_device_heads if by_heads else per_device_gather,
        mesh=mesh,
        in_specs=in_specs,
        out_specs=out_specs,
        check_vma=False,
    )
```

```python
import functools

import jax
import jax.numpy as jnp
from jax import lax
from jax.experimental import pallas as pl
from jax.experimental.pallas import tpu as pltpu
from jax.sharding import PartitionSpec as P

HEADS = 17
HEAD_DIM = 64
MESH = pl.DeviceIdType.MESH


def for_sending(array):

    def short(part):
        return part.astype(jnp.bfloat16) if part.dtype == jnp.float32 else part

    return jax.tree.map(short, array)


def norm_rows(values, gain, shift):
    center = values - jnp.mean(values, -1, keepdims=True)
    spread = jnp.mean(center * center, -1, keepdims=True)
    return center * lax.rsqrt(spread + 1e-05) * gain + shift


def gelu_tanh(values):
    return jax.nn.gelu(values, approximate=True)


def inner_rows(left, right):
    return lax.dot_general(
        left, right, (((0,), (0,)), ((), ())), preferred_element_type=jnp.float32
    )


def times_transposed(left, right):
    return lax.dot_general(
        left, right, (((1,), (1,)), ((), ())), preferred_element_type=jnp.float32
    )


def masked_scores(queries, keys, query_place, key_place, prefix_len, scale):
    scores = jnp.einsum("qhe,khe->hqk", queries, keys, preferred_element_type=jnp.float32) * scale
    allowed = (key_place[None, :] <= query_place[:, None]) | (key_place[None, :] < prefix_len)
    return jnp.where(allowed[None], scores, -1e30)


def reduce_grads(terms):
    owned = jax.tree.map(
        lambda part: part.astype(jnp.float32),
        lax.psum_scatter(for_sending(terms), "group", scatter_dimension=0, tiled=True),
    )
    return jax.tree.map(
        lambda part: part.astype(jnp.float32), lax.psum(for_sending(owned), "replica")
    )


def per_device_gather(
    tokens,
    out_grad,
    positions,
    prefix,
    ln1_gain,
    ln1_bias,
    w_qkv,
    b_query,
    b_value,
    w_attn_out,
    b_attn_out,
    ln2_gain,
    ln2_bias,
    w_fc,
    b_fc,
    w_proj,
    b_proj,
):
    shards = (
        ln1_gain,
        ln1_bias,
        w_qkv,
        b_query,
        b_value,
        w_attn_out,
        b_attn_out,
        ln2_gain,
        ln2_bias,
        w_fc,
        b_fc,
        w_proj,
        b_proj,
    )
    micro = tokens.shape[0]
    rows_here = tokens.shape[2]
    width = tokens.shape[3]
    scale = HEAD_DIM ** (-0.5)
    head_shape = (rows_here, HEADS, HEAD_DIM)
    all_places = lax.all_gather(positions, "replica", axis=2, tiled=True)
    outputs_list = []
    grads_list = []
    kept = None
    owned = None
    for step in range(micro):
        full = (
            lax.all_gather(shards[0], "group", axis=0, tiled=True),
            lax.all_gather(shards[1], "group", axis=0, tiled=True),
            lax.all_gather(shards[2], "group", axis=0, tiled=True),
            lax.all_gather(shards[3], "group", axis=0, tiled=True),
            lax.all_gather(shards[4], "group", axis=0, tiled=True),
            lax.all_gather(shards[5], "group", axis=0, tiled=True),
            lax.all_gather(shards[6], "group", axis=0, tiled=True),
            lax.all_gather(shards[7], "group", axis=0, tiled=True),
            lax.all_gather(shards[8], "group", axis=0, tiled=True),
            lax.all_gather(shards[9], "group", axis=0, tiled=True),
            lax.all_gather(shards[10], "group", axis=0, tiled=True),
            lax.all_gather(shards[11], "group", axis=0, tiled=True),
            lax.all_gather(shards[12], "group", axis=0, tiled=True),
        )
        (
            gain_one,
            shift_one,
            mat_qkv,
            bias_query,
            bias_value,
            mat_out,
            bias_out,
            gain_two,
            shift_two,
            mat_fc,
            bias_fc,
            mat_proj,
            bias_proj,
        ) = full
        gain_one = gain_one.astype(jnp.float32)
        shift_one = shift_one.astype(jnp.float32)
        bias_query = bias_query.astype(jnp.float32)
        bias_value = bias_value.astype(jnp.float32)
        bias_out = bias_out.astype(jnp.float32)
        gain_two = gain_two.astype(jnp.float32)
        shift_two = shift_two.astype(jnp.float32)
        bias_fc = bias_fc.astype(jnp.float32)
        bias_proj = bias_proj.astype(jnp.float32)
        rows_in = tokens[step, 0].astype(jnp.float32)
        query_place = positions[step, 0]
        key_place = all_places[step, 0]
        prefix_len = prefix[step, 0]
        normed_one, norm_one_pull = jax.vjp(norm_rows, rows_in, gain_one, shift_one)
        first = normed_one.astype(jnp.bfloat16)
        joined = jnp.dot(first, mat_qkv, preferred_element_type=jnp.float32)
        queries = (joined[:, :width] + bias_query).astype(jnp.bfloat16)
        keys = joined[:, width : 2 * width].astype(jnp.bfloat16)
        values = (joined[:, 2 * width :] + bias_value).astype(jnp.bfloat16)
        key_all, value_all = (
            lax.all_gather(keys, "replica", axis=0, tiled=True),
            lax.all_gather(values, "replica", axis=0, tiled=True),
        )
        length = key_all.shape[0]
        block = min(512, length)
        nblocks = length // block
        query_heads = queries.reshape(head_shape)
        key_blocks = key_all.reshape(nblocks, block, HEADS, HEAD_DIM)
        value_blocks = value_all.reshape(nblocks, block, HEADS, HEAD_DIM)
        place_blocks = key_place.reshape(nblocks, block)

        def attend_step(carry, blockargs):
            highest, total, summed = carry
            key_part, value_part, place_part = blockargs
            scores = masked_scores(
                query_heads, key_part, query_place, place_part, prefix_len, scale
            )
            new_high = jnp.maximum(highest, jnp.max(scores, -1))
            factor = jnp.exp(highest - new_high)
            expo = jnp.exp(scores - new_high[..., None])
            total = total * factor + jnp.sum(expo, -1)
            summed = summed * jnp.transpose(factor)[..., None] + jnp.einsum(
                "hqk,khe->qhe",
                expo.astype(jnp.bfloat16),
                value_part,
                preferred_element_type=jnp.float32,
            )
            return ((new_high, total, summed), None)

        start_carry = (
            jnp.full((HEADS, rows_here), -1e30, jnp.float32),
            jnp.zeros((HEADS, rows_here), jnp.float32),
            jnp.zeros(head_shape, jnp.float32),
        )
        (highest, total, summed), _ = lax.scan(
            attend_step, start_carry, (key_blocks, value_blocks, place_blocks)
        )
        log_total = highest + jnp.log(total)
        attended_f = summed / jnp.transpose(total)[..., None]
        attended = attended_f.reshape(rows_here, width).astype(jnp.bfloat16)
        middle = rows_in + jnp.dot(attended, mat_out, preferred_element_type=jnp.float32) + bias_out
        normed_two, norm_two_pull = jax.vjp(norm_rows, middle, gain_two, shift_two)
        second = normed_two.astype(jnp.bfloat16)
        hidden_in = jnp.dot(second, mat_fc, preferred_element_type=jnp.float32) + bias_fc
        hidden_f, gelu_pull = jax.vjp(gelu_tanh, hidden_in)
        hidden = hidden_f.astype(jnp.bfloat16)
        output_rows = (
            middle + jnp.dot(hidden, mat_proj, preferred_element_type=jnp.float32) + bias_proj
        )
        outputs_list.append(output_rows.astype(jnp.bfloat16))
        grad_top = out_grad[step, 0].astype(jnp.float32)
        grad_low = out_grad[step, 0]
        grad_bias_proj = jnp.sum(grad_top, 0)
        grad_mat_proj = inner_rows(hidden, grad_low)
        grad_hidden = times_transposed(grad_low, mat_proj)
        (grad_hidden_in,) = gelu_pull(grad_hidden)
        grad_hidden_in = grad_hidden_in.astype(jnp.bfloat16)
        grad_bias_fc = jnp.sum(grad_hidden_in, 0, dtype=jnp.float32)
        grad_mat_fc = inner_rows(second, grad_hidden_in)
        grad_second = times_transposed(grad_hidden_in, mat_fc)
        grad_middle_norm, grad_gain_two, grad_shift_two = norm_two_pull(grad_second)
        grad_middle = grad_top + grad_middle_norm
        grad_bias_out = jnp.sum(grad_middle, 0)
        grad_branch = grad_middle.astype(jnp.bfloat16)
        grad_mat_out = inner_rows(attended, grad_branch)
        grad_attended = times_transposed(grad_branch, mat_out).astype(jnp.bfloat16)
        grad_heads = grad_attended.reshape(head_shape)
        delta = jnp.transpose(jnp.sum(grad_heads.astype(jnp.float32) * attended_f, -1))

        def score_grads(
            query_part, grad_part, key_part, value_part, qplace, kplace, lse_part, delta_part
        ):
            scores = masked_scores(query_part, key_part, qplace, kplace, prefix_len, scale)
            probs = jnp.exp(scores - lse_part[..., None])
            grad_probs = jnp.einsum(
                "qhe,khe->hqk", grad_part, value_part, preferred_element_type=jnp.float32
            )
            grad_scores = (probs * (grad_probs - delta_part[..., None])).astype(jnp.bfloat16)
            return (probs.astype(jnp.bfloat16), grad_scores)

        def grad_step(summed, blockargs):
            key_part, value_part, place_part = blockargs
            probs, grad_scores = score_grads(
                query_heads,
                grad_heads,
                key_part,
                value_part,
                query_place,
                place_part,
                log_total,
                delta,
            )
            summed = summed + jnp.einsum(
                "hqk,khe->qhe", grad_scores, key_part, preferred_element_type=jnp.float32
            )
            key_grad = jnp.einsum(
                "hqk,qhe->khe", grad_scores, query_heads, preferred_element_type=jnp.float32
            )
            value_grad = jnp.einsum(
                "hqk,qhe->khe", probs, grad_heads, preferred_element_type=jnp.float32
            )
            return (summed, (key_grad, value_grad))

        grad_query, (key_grads, value_grads) = lax.scan(
            grad_step, jnp.zeros(head_shape, jnp.float32), (key_blocks, value_blocks, place_blocks)
        )
        grad_key, grad_value = (
            lax.psum_scatter(
                key_grads.reshape(length, width).astype(jnp.bfloat16),
                "replica",
                scatter_dimension=0,
                tiled=True,
            ).astype(jnp.float32),
            lax.psum_scatter(
                value_grads.reshape(length, width).astype(jnp.bfloat16),
                "replica",
                scatter_dimension=0,
                tiled=True,
            ).astype(jnp.float32),
        )
        grad_query = (grad_query.reshape(rows_here, width) * scale).astype(jnp.bfloat16)
        grad_key = (grad_key * scale).astype(jnp.bfloat16)
        grad_value = grad_value.astype(jnp.bfloat16)
        grad_bias_query = jnp.sum(grad_query, 0, dtype=jnp.float32)
        grad_bias_value = jnp.sum(grad_value, 0, dtype=jnp.float32)
        grad_joined = jnp.concatenate([grad_query, grad_key, grad_value], 1)
        grad_mat_qkv = inner_rows(first, grad_joined)
        grad_first = times_transposed(grad_joined, mat_qkv)
        grad_rows_norm, grad_gain_one, grad_shift_one = norm_one_pull(grad_first)
        grads_list.append((grad_middle + grad_rows_norm).astype(jnp.bfloat16))
        terms = (
            grad_gain_one,
            grad_shift_one,
            grad_mat_qkv,
            grad_bias_query,
            grad_bias_value,
            grad_mat_out,
            grad_bias_out,
            grad_gain_two,
            grad_shift_two,
            grad_mat_fc,
            grad_bias_fc,
            grad_mat_proj,
            grad_bias_proj,
        )
        kept = (
            terms
            if kept is None
            else tuple((first_term + second_term for first_term, second_term in zip(kept, terms)))
        )
    owned = reduce_grads(kept)
    result = jnp.stack(outputs_list).reshape(micro, 1, rows_here, width)
    tokens_grad = jnp.stack(grads_list).reshape(micro, 1, rows_here, width)
    return (result, tokens_grad) + tuple(owned)


def contract(left, right, left_dim, right_dim):
    return lax.dot_general(
        left, right, (((left_dim,), (right_dim,)), ((), ())), preferred_element_type=jnp.float32
    )


def greet(peers, here, group_too):
    barrier = pltpu.get_barrier_semaphore()

    def one(step, carry):
        peer = lax.rem(here + step, peers)
        pl.semaphore_signal(barrier, inc=1, device_id={"replica": peer}, device_id_type=MESH)
        return carry

    lax.fori_loop(1, peers, one, 0)
    if group_too:
        other = 1 - lax.axis_index("group")
        pl.semaphore_signal(barrier, inc=1, device_id={"group": other}, device_id_type=MESH)
    pl.semaphore_wait(barrier, peers - 1 + (1 if group_too else 0))


def halves(ref, mode, which):
    if mode == "whole":
        return ref
    if mode == "rows":
        size = ref.shape[0] // 2
        return ref.at[pl.ds(pl.multiple_of(which * size, 16), size)]
    size = ref.shape[1] // 2
    return ref.at[:, pl.ds(pl.multiple_of(which * size, 128), size)]


def half_shape(array, mode):
    rows, columns = array.shape
    return {"whole": (rows, columns), "rows": (rows // 2, columns), "columns": (rows, columns // 2)}[mode]


def exchange_body(direction, with_places, modes, *refs):
    refs = list(refs)
    nweights = len(modes)
    chunk, last = refs.pop(0), refs.pop(0)
    places = refs.pop(0) if with_places else None
    weights = [refs.pop(0) for _ in range(nweights)]
    chunk_out, last_out = refs.pop(0), refs.pop(0)
    places_out = refs.pop(0) if with_places else None
    weights_out = [refs.pop(0) for _ in range(nweights)]
    send, recv, last_send, last_recv, own = (refs.pop(0) for _ in range(5))
    if with_places:
        place_send, place_recv = refs.pop(0), refs.pop(0)
    if nweights:
        weight_send, weight_recv, weight_own = (refs.pop(0) for _ in range(3))
        bounce = [refs.pop(0) for _ in range(nweights)]
    peers = chunk.shape[0]
    here = lax.axis_index("replica")
    group = lax.axis_index("group")
    greet(peers, here, nweights > 0)
    loads, copies = [], []
    for i in range(nweights):
        copy = pltpu.make_async_remote_copy(
            halves(weights[i], modes[i], 1 - group),
            weights_out[i].at[group],
            weight_send.at[i],
            weight_recv.at[i],
            device_id={"group": 1 - group},
            device_id_type=MESH,
        )
        copy.start()
        copies.append(copy)
        load = pltpu.make_async_copy(
            halves(weights[i], modes[i], group), bounce[i], weight_own.at[i]
        )
        load.start()
        loads.append(load)
    for slot in range(2):
        half = peers // 2
        target = lax.rem(here + direction + peers, half) + half * slot
        copy = pltpu.make_async_remote_copy(
            last.at[slot],
            last_out.at[here // half],
            last_send.at[slot],
            last_recv.at[here // half],
            device_id={"replica": target},
            device_id_type=MESH,
        )
        copy.start()
        copies.append(
            (
                copy,
                pltpu.make_async_remote_copy(
                    last.at[slot],
                    last_out.at[slot],
                    last_send.at[slot],
                    last_recv.at[slot],
                    device_id={"replica": target},
                    device_id_type=MESH,
                ),
            )
        )
    for step in range(1, peers):
        peer = lax.rem(here + step, peers)
        copy = pltpu.make_async_remote_copy(
            chunk.at[peer],
            chunk_out.at[here],
            send.at[step],
            recv.at[step],
            device_id={"replica": peer},
            device_id_type=MESH,
        )
        copy.start()
        copies.append(copy)
        if with_places:
            copy = pltpu.make_async_remote_copy(
                places,
                places_out.at[here],
                place_send.at[step],
                place_recv.at[step],
                device_id={"replica": peer},
                device_id_type=MESH,
            )
            copy.start()
            copies.append(copy)
    owns = [pltpu.make_async_copy(chunk.at[here], chunk_out.at[here], own.at[0])]
    if with_places:
        owns.append(pltpu.make_async_copy(places, places_out.at[here], own.at[1]))
    for copy in owns:
        copy.start()
    stores = []
    for i, load in enumerate(loads):
        load.wait()
        store = pltpu.make_async_copy(bounce[i], weights_out[i].at[group], weight_own.at[i])
        store.start()
        stores.append(store)
    for copy in stores + owns:
        copy.wait()
    for copy in copies:
        if isinstance(copy, tuple):
            copy[0].wait_send()
            copy[1].wait_recv()
        else:
            copy.wait()


def exchange(ident, direction, chunk, last, places=None, shares=()):
    peers = chunk.shape[0]
    weights = [array for array, _ in shares]
    modes = [mode for _, mode in shares]
    any_spec = pl.BlockSpec(memory_space=pl.ANY)
    with_places = places is not None
    args = [chunk, last] + ([places] if with_places else []) + list(weights)
    shapes = [(chunk.shape, chunk.dtype), (last.shape, last.dtype)]
    if with_places:
        shapes.append(((peers,) + places.shape, places.dtype))
    shapes += [((2,) + half_shape(*item), item[0].dtype) for item in shares]
    dma = pltpu.SemaphoreType.DMA
    scratch = [dma((peers,)), dma((peers,)), dma((2,)), dma((2,)), dma((2,))]
    if with_places:
        scratch += [dma((peers,)), dma((peers,))]
    if weights:
        count = len(weights)
        scratch += [dma((count,)), dma((count,)), dma((count,))]
        scratch += [pltpu.VMEM(half_shape(*item), item[0].dtype) for item in shares]
    return pl.pallas_call(
        functools.partial(exchange_body, direction, with_places, modes),
        out_shape=[jax.ShapeDtypeStruct(*shape) for shape in shapes],
        in_specs=[any_spec] * len(args),
        out_specs=[any_spec] * len(shapes),
        scratch_shapes=scratch,
        compiler_params=pltpu.CompilerParams(collective_id=ident, has_side_effects=True),
        name=f"exchange{ident}",
    )(*args)


def share_body(count, *refs):
    sources, results = refs[:count], refs[count : 2 * count]
    send, recv, own = refs[2 * count : 2 * count + 3]
    bounce = refs[2 * count + 3 :]
    group = lax.axis_index("group")
    barrier = pltpu.get_barrier_semaphore()
    pl.semaphore_signal(barrier, inc=1, device_id={"group": 1 - group}, device_id_type=MESH)
    pl.semaphore_wait(barrier, 1)
    copies, loads, stores = [], [], []
    for i in range(count):
        copy = pltpu.make_async_remote_copy(
            sources[i],
            results[i].at[group],
            send.at[i],
            recv.at[i],
            device_id={"group": 1 - group},
            device_id_type=MESH,
        )
        copy.start()
        copies.append(copy)
        load = pltpu.make_async_copy(sources[i], bounce[i], own.at[i])
        load.start()
        loads.append(load)
    for i in range(count):
        loads[i].wait()
        store = pltpu.make_async_copy(bounce[i], results[i].at[group], own.at[i])
        store.start()
        stores.append(store)
    for copy in stores + copies:
        copy.wait()


def share(ident, *arrays):
    count = len(arrays)
    any_spec = pl.BlockSpec(memory_space=pl.ANY)
    dma = pltpu.SemaphoreType.DMA
    return pl.pallas_call(
        functools.partial(share_body, count),
        out_shape=[jax.ShapeDtypeStruct((2,) + a.shape, a.dtype) for a in arrays],
        in_specs=[any_spec] * count,
        out_specs=[any_spec] * count,
        scratch_shapes=[dma((count,)), dma((count,)), dma((count,))]
        + [pltpu.VMEM(a.shape, a.dtype) for a in arrays],
        compiler_params=pltpu.CompilerParams(collective_id=ident, has_side_effects=True),
        name=f"share{ident}",
    )(*arrays)


BLOCK = 256


def unpack_units(got, last, rows_at, query_out):
    peers = got.shape[0]
    half = BLOCK // 128
    for m in range(2):
        for s in range(peers):
            query_out[m * (peers // half) + s // half, :, (s % half) * 128 : (s % half + 1) * 128] = got[
                s, rows_at : rows_at + 64, m * 128 : (m + 1) * 128
            ]
    extra = 2 * (peers // half)
    for j in range(2):
        query_out[extra, :, j * 128 : (j + 1) * 128] = last[j]


def unit_source(got, u, s, first):
    if u < 2:
        return got[s, first : first + 64, u * 128 : (u + 1) * 128]
    at = 0 if first == 64 else 128
    return got[s, 192:256, at : at + 128]


def attend_body(got, last, limit, places, sent, last_sent, out_f, lse, keys, values, queries, outs):
    peers = got.shape[0]
    nblocks = queries.shape[0]
    per_unit = (nblocks - 1) // 2
    unpack_units(got, last, 0, queries)
    for u in range(3):
        for s in range(peers):
            span = slice(s * 128, (s + 1) * 128)
            keys[u, span, :] = unit_source(got, u, s, 64).T
            values[u, :, span] = unit_source(got, u, s, 128)

    def block(b, carry):
        u = b // per_unit
        scores = jnp.dot(keys[u], queries[b], preferred_element_type=jnp.float32)
        place = places[u]
        place = jnp.concatenate([place, place], axis=1)
        scores = jnp.where(place < limit[b], scores, -1e30)
        high = jnp.max(scores, axis=0, keepdims=True)
        expo = jnp.exp(scores - high)
        total = jnp.sum(expo, axis=0, keepdims=True)
        summed = jnp.dot(values[u], expo.astype(jnp.bfloat16), preferred_element_type=jnp.float32)
        result = summed / total
        out_f[b] = result
        outs[b] = result.astype(jnp.bfloat16)
        lse[b] = high + jnp.log(total)
        return carry

    lax.fori_loop(0, nblocks, block, 0)
    half = BLOCK // 128
    for m in range(2):
        for s in range(peers):
            sent[s, :, m * 128 : (m + 1) * 128] = outs[
                m * per_unit + s // half, :, (s % half) * 128 : (s % half + 1) * 128
            ]
    for j in range(2):
        last_sent[j] = outs[nblocks - 1, :, j * 128 : (j + 1) * 128]


def attend(got, last, limit, places):
    peers = got.shape[0]
    nblocks = limit.shape[0]
    length = places.shape[1]
    bf, f32 = jnp.bfloat16, jnp.float32
    return pl.pallas_call(
        attend_body,
        out_shape=[
            jax.ShapeDtypeStruct((peers, 64, 256), bf),
            jax.ShapeDtypeStruct((2, 64, 128), bf),
            jax.ShapeDtypeStruct((nblocks, 64, BLOCK), f32),
            jax.ShapeDtypeStruct((nblocks, 1, BLOCK), f32),
        ],
        scratch_shapes=[
            pltpu.VMEM((3, length, 64), bf),
            pltpu.VMEM((3, 64, length), bf),
            pltpu.VMEM((nblocks, 64, BLOCK), bf),
            pltpu.VMEM((nblocks, 64, BLOCK), bf),
        ],
        compiler_params=pltpu.CompilerParams(vmem_limit_bytes=56 << 20),
        name="attend",
    )(got, last, limit, places)


def attend_grad_body(
    got,
    last,
    limit,
    places,
    out_f,
    lse,
    grad_got,
    grad_last,
    sent,
    last_sent,
    keys,
    keys_t,
    values,
    queries,
    grads,
    queries_n,
    grads_n,
    dqs,
    dk,
    dv,
):
    peers = got.shape[0]
    nblocks = queries.shape[0]
    per_unit = (nblocks - 1) // 2
    unpack_units(got, last, 0, queries)
    unpack_units(grad_got, grad_last, 0, grads)
    for u in range(3):
        for s in range(peers):
            span = slice(s * 128, (s + 1) * 128)
            part = unit_source(got, u, s, 64)
            keys[u, span, :] = part.T
            keys_t[u, :, span] = part
            values[u, span, :] = unit_source(got, u, s, 128).T
    for b in range(nblocks):
        queries_n[b] = queries[b].T
        grads_n[b] = grads[b].T
    dk[...] = jnp.zeros_like(dk)
    dv[...] = jnp.zeros_like(dv)

    def block(b, carry):
        u = b // per_unit
        grad = grads[b]
        delta = jnp.sum(grad.astype(jnp.float32) * out_f[b], axis=0, keepdims=True)
        scores = jnp.dot(keys[u], queries[b], preferred_element_type=jnp.float32)
        place = places[u]
        place = jnp.concatenate([place, place], axis=1)
        scores = jnp.where(place < limit[b], scores, -1e30)
        probs = jnp.exp(scores - lse[b])
        grad_probs = jnp.dot(values[u], grad, preferred_element_type=jnp.float32)
        grad_scores = (probs * (grad_probs - delta)).astype(jnp.bfloat16)
        dqs[b] = jnp.dot(keys_t[u], grad_scores, preferred_element_type=jnp.float32)
        dk[u] += jnp.dot(grad_scores, queries_n[b], preferred_element_type=jnp.float32)
        dv[u] += jnp.dot(probs.astype(jnp.bfloat16), grads_n[b], preferred_element_type=jnp.float32)
        return carry

    lax.fori_loop(0, nblocks, block, 0)
    half = BLOCK // 128
    scale = HEAD_DIM ** (-0.5)
    for m in range(2):
        for s in range(peers):
            at = slice(m * 128, (m + 1) * 128)
            span = slice(s * 128, (s + 1) * 128)
            dq = dqs[m * per_unit + s // half, :, (s % half) * 128 : (s % half + 1) * 128]
            sent[s, 0:64, at] = (dq * scale).astype(jnp.bfloat16)
            sent[s, 64:128, at] = dk[m, span, :].T.astype(jnp.bfloat16)
            sent[s, 128:192, at] = dv[m, span, :].T.astype(jnp.bfloat16)
    for s in range(peers):
        span = slice(s * 128, (s + 1) * 128)
        sent[s, 192:256, 0:128] = dk[2, span, :].T.astype(jnp.bfloat16)
        sent[s, 192:256, 128:256] = dv[2, span, :].T.astype(jnp.bfloat16)
    for j in range(2):
        last_sent[j] = (dqs[nblocks - 1, :, j * 128 : (j + 1) * 128] * scale).astype(jnp.bfloat16)


def attend_grad(got, last, limit, places, out_f, lse, grad_got, grad_last):
    peers = got.shape[0]
    nblocks = limit.shape[0]
    length = places.shape[1]
    bf, f32 = jnp.bfloat16, jnp.float32
    return pl.pallas_call(
        attend_grad_body,
        out_shape=[
            jax.ShapeDtypeStruct((peers, 256, 256), bf),
            jax.ShapeDtypeStruct((2, 64, 128), bf),
        ],
        scratch_shapes=[
            pltpu.VMEM((3, length, 64), bf),
            pltpu.VMEM((3, 64, length), bf),
            pltpu.VMEM((3, length, 64), bf),
            pltpu.VMEM((nblocks, 64, BLOCK), bf),
            pltpu.VMEM((nblocks, 64, BLOCK), bf),
            pltpu.VMEM((nblocks, BLOCK, 64), bf),
            pltpu.VMEM((nblocks, BLOCK, 64), bf),
            pltpu.VMEM((nblocks, 64, BLOCK), f32),
            pltpu.VMEM((3, length, 64), f32),
            pltpu.VMEM((3, length, 64), f32),
        ],
        compiler_params=pltpu.CompilerParams(vmem_limit_bytes=60 << 20),
        name="attend_grad",
    )(got, last, limit, places, out_f, lse, grad_got, grad_last)


ROWS = 272
PART = 80
PADDED = 4 * PART


def chunk_plan(wide_widths, tall_widths):
    plan = []
    for array in (2, 0, 1):
        if array == 2:
            for row in (0, ROWS):
                start = 0
                for width in tall_widths:
                    plan.append((2, width, row, start))
                    start += width
        else:
            start = 0
            for width in wide_widths:
                plan.append((array, width, 0, start))
                start += width
    return plan


def piece(ref, item, first, second):
    array, width, row, start = item
    if array == 2:
        at = first * (4 * ROWS) + second * (2 * ROWS) + row
        return ref.at[pl.ds(pl.multiple_of(at, 16), ROWS), pl.ds(start, width)]
    column = pl.multiple_of(second * 2176 + start, 128)
    return ref.at[pl.ds(pl.multiple_of(first * ROWS, 16), ROWS), pl.ds(column, width)]


def sum_grads_body(plan, *refs):
    nchunks = len(plan)
    sources, small, results, small_out = refs[0:3], refs[3], refs[4:7], refs[7]
    refs = list(refs[8:])
    own, came, second_in, quarter, parts, gathered, other = (
        [refs.pop(0) for _ in range(nchunks)] for _ in range(7)
    )
    small_half, small_sum, small_all = (refs.pop(0) for _ in range(3))
    (load_sem, s1, r1, s2, r2, s3, r3, s4, r4, s5, r5, s6, r6, store_sem, sp, rp, sa, ra) = refs
    here, group = lax.axis_index("replica"), lax.axis_index("group")
    peers = small_all.shape[0]
    bit_x, bit_y, place = here % 2, (here // 2) % 2, here // 4
    bit_one = bit_x + group * (bit_y - bit_x)
    bit_two = bit_x + bit_y - bit_one
    peer_one = here + (1 + group) * (1 - 2 * bit_one)
    peer_two = here + (2 - group) * (1 - 2 * bit_two)
    greet(peers, here, True)
    pending = []

    def send(source, target, send_sem, recv_sem, peer):
        copy = pltpu.make_async_remote_copy(
            source, target, send_sem, recv_sem, device_id={"replica": peer}, device_id_type=MESH
        )
        copy.start()
        pending.append(copy)
        return copy

    small_copy = pltpu.make_async_remote_copy(
        small.at[1 - group],
        small_half,
        sp,
        rp,
        device_id={"group": 1 - group},
        device_id_type=MESH,
    )
    small_copy.start()
    first_copies, loads = [], []
    for c, item in enumerate(plan):
        source = sources[item[0]]
        group_of = []
        for j in range(2):
            group_of.append(
                send(
                    piece(source, item, 1 - bit_one, j),
                    came[c].at[j],
                    s1.at[c, j],
                    r1.at[c, j],
                    peer_one,
                )
            )
        first_copies.append(group_of)
        pair = []
        for j in range(2):
            load = pltpu.make_async_copy(
                piece(source, item, bit_one, j), own[c].at[j], load_sem.at[c, j]
            )
            load.start()
            pair.append(load)
        loads.append(pair)
    for c in range(nchunks):
        quarter[c][ROWS:, :] = jnp.zeros((PADDED - ROWS, quarter[c].shape[1]), jnp.bfloat16)
    small_copy.wait()
    small_sum[...] = small[group] + small_half[...]
    small_all[here] = small_sum[...]
    small_copies = []
    for step in range(1, peers):
        copy = pltpu.make_async_remote_copy(
            small_sum,
            small_all.at[here],
            sa.at[step],
            ra.at[step],
            device_id={"replica": lax.rem(here + step, peers)},
            device_id_type=MESH,
        )
        copy.start()
        small_copies.append(copy)

    def by_rows(rows, fn):
        lax.fori_loop(0, rows // 16, lambda i, carry: (fn(pl.ds(pl.multiple_of(i * 16, 16), 16)), carry)[1], 0)

    second_copies, part_copies, gather_copies, other_copies, last_copies = {}, {}, {}, {}, {}
    stores = []

    def stage_one(c):
        for j in range(2):
            loads[c][j].wait()
            first_copies[c][j].wait_recv()

        def add(rows):
            both = own[c][1 - bit_two, rows].astype(jnp.float32) + came[c][
                1 - bit_two, rows
            ].astype(jnp.float32)
            own[c][1 - bit_two, rows] = both.astype(jnp.bfloat16)

        by_rows(ROWS, add)
        second_copies[c] = send(
            own[c].at[1 - bit_two], second_in[c], s2.at[c], r2.at[c], peer_two
        )

    def stage_two(c):
        second_copies[c].wait_recv()

        def add(rows):
            total = own[c][bit_two, rows].astype(jnp.float32) + came[c][bit_two, rows].astype(
                jnp.float32
            )
            total = total + second_in[c][rows].astype(jnp.float32)
            quarter[c][rows] = total.astype(jnp.bfloat16)

        by_rows(ROWS, add)
        part_copies[c] = [
            send(
                quarter[c].at[pl.ds(pl.multiple_of(lax.rem(place + k, 4) * PART, 16), PART)],
                parts[c].at[k - 1],
                s3.at[c, k - 1],
                r3.at[c, k - 1],
                lax.rem(here + 4 * k, peers),
            )
            for k in (1, 2, 3)
        ]

    def stage_three(c):
        for copy in part_copies[c]:
            copy.wait_recv()

        def add(rows):
            at = pl.ds(pl.multiple_of(place * PART + rows.start, 16), 16)
            total = quarter[c][at].astype(jnp.float32)
            for k in range(3):
                total = total + parts[c][k, rows].astype(jnp.float32)
            gathered[c][at] = total.astype(jnp.bfloat16)

        by_rows(PART, add)
        block = pl.ds(pl.multiple_of(place * PART, 16), PART)
        gather_copies[c] = [
            send(
                gathered[c].at[block],
                gathered[c].at[block],
                s4.at[c, k - 1],
                r4.at[c, k - 1],
                lax.rem(here + 4 * k, peers),
            )
            for k in (1, 2, 3)
        ]

    def stage_four(c):
        item = plan[c]
        result = results[item[0]]
        for copy in gather_copies[c]:
            copy.wait_recv()
        whole = gathered[c].at[pl.ds(0, ROWS)]
        other_copies[c] = send(whole, other[c], s5.at[c], r5.at[c], peer_two)
        last_copies[c] = [
            send(whole, piece(result, item, bit_one, bit_two), s6.at[c, 0], r6.at[c, 0], peer_one)
        ]
        store = pltpu.make_async_copy(
            whole, piece(result, item, bit_one, bit_two), store_sem.at[c, 0]
        )
        store.start()
        stores.append(store)

    def stage_five(c):
        item = plan[c]
        result = results[item[0]]
        other_copies[c].wait_recv()
        last_copies[c].append(
            send(
                other[c],
                piece(result, item, bit_one, 1 - bit_two),
                s6.at[c, 1],
                r6.at[c, 1],
                peer_one,
            )
        )
        store = pltpu.make_async_copy(
            other[c], piece(result, item, bit_one, 1 - bit_two), store_sem.at[c, 1]
        )
        store.start()
        stores.append(store)

    stages = (stage_one, stage_two, stage_three, stage_four, stage_five)
    for tick in range(nchunks + len(stages) - 1):
        for number in reversed(range(len(stages))):
            c = tick - number
            if 0 <= c < nchunks:
                stages[number](c)
    for copy in small_copies:
        copy.wait()
    total = small_all[0]
    for i in range(1, peers):
        total = total + small_all[i]
    small_out[...] = total
    for c in range(nchunks):
        for copy in last_copies[c]:
            copy.wait_recv()
    for copy in pending:
        copy.wait_send()
    for store in stores:
        store.wait()


def sum_grads(ident, grad_fc, grad_rest, grad_proj, small):
    plan = chunk_plan((1152, 1024), (1088,))
    nchunks = len(plan)
    peers = lax.axis_size("replica")
    bf, f32 = jnp.bfloat16, jnp.float32
    any_spec = pl.BlockSpec(memory_space=pl.ANY)
    vmem = pl.BlockSpec(memory_space=pltpu.VMEM)
    dma = pltpu.SemaphoreType.DMA
    arrays = (grad_fc, grad_rest, grad_proj)
    buffers = []
    for shape in (
        lambda w: (2, ROWS, w),
        lambda w: (2, ROWS, w),
        lambda w: (ROWS, w),
        lambda w: (PADDED, w),
        lambda w: (3, PART, w),
        lambda w: (PADDED, w),
        lambda w: (ROWS, w),
    ):
        buffers += [pltpu.VMEM(shape(item[1]), bf) for item in plan]
    one_small = small.shape[1:]
    buffers += [
        pltpu.VMEM(one_small, f32),
        pltpu.VMEM(one_small, f32),
        pltpu.VMEM((peers,) + one_small, f32),
    ]
    pairs, triples, ones = dma((nchunks, 2)), dma((nchunks, 3)), dma((nchunks,))
    sems = [pairs, pairs, pairs, ones, ones, triples, triples, triples, triples, ones, ones]
    sems += [pairs, pairs, pairs, dma, dma, dma((peers,)), dma((peers,))]
    return pl.pallas_call(
        functools.partial(sum_grads_body, plan),
        out_shape=[jax.ShapeDtypeStruct(a.shape, bf) for a in arrays]
        + [jax.ShapeDtypeStruct(one_small, f32)],
        in_specs=[any_spec] * 3 + [vmem],
        out_specs=[any_spec] * 3 + [vmem],
        scratch_shapes=buffers + sems,
        compiler_params=pltpu.CompilerParams(
            collective_id=ident, has_side_effects=True, vmem_limit_bytes=56 << 20
        ),
        name=f"sum_grads{ident}",
    )(*arrays, small)


def split_last(array):
    return jnp.stack([array[:, :128], array[:, 128:]])


def per_device_heads(
    tokens,
    out_grad,
    positions,
    prefix,
    ln1_gain,
    ln1_bias,
    w_qkv,
    b_query,
    b_value,
    w_attn_out,
    b_attn_out,
    ln2_gain,
    ln2_bias,
    w_fc,
    b_fc,
    w_proj,
    b_proj,
):
    bf, f32 = jnp.bfloat16, jnp.float32
    micro, _, rows_here, width = tokens.shape
    peers = lax.axis_size("replica")
    hidden_width = 2 * b_fc.shape[0]
    half = peers // 2
    count = micro * rows_here
    here = lax.axis_index("replica")
    scale = HEAD_DIM ** (-0.5)
    split = (peers * HEAD_DIM, width)

    small = jnp.concatenate(
        [ln1_gain, ln1_bias, b_query, b_value, b_attn_out, ln2_gain, ln2_bias, b_proj, b_fc]
    ).reshape(1, -1)
    mat_qkv, vectors = share(1, w_qkv, small)
    mat_qkv = mat_qkv.reshape(width, 3 * width)
    vectors = vectors[:, 0].astype(f32)
    part = width // 2
    gain_one, shift_one, bias_query, bias_value, bias_out, gain_two, shift_two, bias_proj = (
        vectors[:, i * part : (i + 1) * part].reshape(width) for i in range(8)
    )
    bias_fc = vectors[:, 8 * part :].reshape(hidden_width)

    rows_in = tokens.reshape(count, width).astype(f32)
    normed_one, norm_one_pull = jax.vjp(norm_rows, rows_in, gain_one, shift_one)
    first = normed_one.astype(bf)
    joined = contract(mat_qkv, first, 0, 1)
    bias_all = jnp.concatenate([bias_query, jnp.zeros_like(bias_query), bias_value])
    joined = joined + bias_all[:, None]
    queries = ((joined[:width]).astype(bf).astype(f32) * scale).astype(bf)
    keys = joined[width : 2 * width].astype(bf)
    values = joined[2 * width :].astype(bf)
    cut = split[0]
    main = [part_[:cut].reshape(peers, HEAD_DIM, count) for part_ in (queries, keys, values)]
    key_last, value_last = keys[cut:], values[cut:]
    tails = jnp.stack(
        [
            jnp.concatenate(
                [key_last[:, m * 128 : (m + 1) * 128], value_last[:, m * 128 : (m + 1) * 128]], 1
            )
            for m in range(2)
        ]
    )
    tails = jnp.repeat(tails, half, axis=0)
    chunk = jnp.concatenate(main + [tails], axis=1)
    grad_low = out_grad.reshape(count, width)
    got, got_last, all_places, mat_out, mat_fc, mat_proj, firsts, grad_lows = exchange(
        2,
        1,
        chunk,
        split_last(queries[cut:]),
        positions.reshape(micro, rows_here),
        [(item, "whole") for item in (w_attn_out, w_fc, w_proj, first, grad_low)],
    )
    mat_out = mat_out.reshape(width, width)
    mat_fc = mat_fc.reshape(width, hidden_width)
    mat_proj = mat_proj.reshape(hidden_width, width)

    place_rows = jnp.transpose(all_places, (1, 0, 2)).reshape(micro, peers * rows_here)
    limits = jnp.maximum(place_rows + 1, prefix.reshape(micro, 1))
    mine = here // half
    at = lax.rem(here - 1 + peers, half)
    own_limits = lax.dynamic_index_in_dim(limits, mine, 0, False).reshape(peers, rows_here)
    own_limits = jnp.concatenate(
        [
            lax.dynamic_index_in_dim(own_limits, at, 0, True),
            lax.dynamic_index_in_dim(own_limits, at + half, 0, True),
        ],
        1,
    )
    limit = jnp.concatenate([limits.reshape(-1, BLOCK), own_limits], 0)[:, None, :]
    unit_places = jnp.concatenate(
        [place_rows, lax.dynamic_index_in_dim(place_rows, mine, 0, True)], 0
    )
    unit_places = jnp.broadcast_to(unit_places[:, :, None], unit_places.shape + (128,))

    sent, sent_last, out_f, lse = attend(got, got_last, limit, unit_places)
    heads_out, heads_last = exchange(3, -1, sent, sent_last)
    attended = jnp.concatenate(
        [heads_out.reshape(cut, count), jnp.concatenate([heads_last[0], heads_last[1]], 1)], 0
    )

    middle = rows_in + contract(attended, mat_out, 0, 0) + bias_out
    normed_two, norm_two_pull = jax.vjp(norm_rows, middle, gain_two, shift_two)
    second = normed_two.astype(bf)
    hidden_in = jnp.dot(second, mat_fc, preferred_element_type=f32) + bias_fc
    hidden_f, gelu_pull = jax.vjp(gelu_tanh, hidden_in)
    hidden = hidden_f.astype(bf)
    output_rows = middle + jnp.dot(hidden, mat_proj, preferred_element_type=f32) + bias_proj
    result = output_rows.astype(bf).reshape(micro, 1, rows_here, width)

    grad_top = grad_low.astype(f32)
    grad_bias_proj = jnp.sum(grad_top, 0)
    (grad_hidden_in,) = gelu_pull(times_transposed(grad_low, mat_proj))
    grad_hidden_in = grad_hidden_in.astype(bf)
    grad_bias_fc = jnp.sum(grad_hidden_in, 0, dtype=f32)
    grad_second = times_transposed(grad_hidden_in, mat_fc)
    grad_middle_norm, grad_gain_two, grad_shift_two = norm_two_pull(grad_second)
    grad_middle = grad_top + grad_middle_norm
    grad_bias_out = jnp.sum(grad_middle, 0)
    grad_branch = grad_middle.astype(bf)
    grad_attended = contract(mat_out, grad_branch, 1, 1).astype(bf)

    grad_got, grad_got_last, hiddens, seconds, grad_ins, attendeds, branches = exchange(
        4,
        1,
        grad_attended[:cut].reshape(peers, HEAD_DIM, count),
        split_last(grad_attended[cut:]),
        None,
        [
            (hidden, "columns"),
            (second, "whole"),
            (grad_hidden_in, "whole"),
            (attended, "rows"),
            (grad_branch, "whole"),
        ],
    )
    group = lax.axis_index("group")

    def own_columns(pair):
        return lax.dynamic_slice_in_dim(pair, group * part, part, 2)

    def both(left, right, left_dims, right_dims):
        return lax.dot_general(
            left, right, ((left_dims, right_dims), ((), ())), preferred_element_type=f32
        ).astype(bf)

    grad_mat_proj = both(hiddens, grad_lows, (0, 1), (0, 1))
    grad_mat_fc = both(own_columns(seconds), grad_ins, (0, 1), (0, 1))
    grad_mat_out = both(attendeds, branches, (0, 2), (0, 1))

    grad_sent, grad_sent_last = attend_grad(
        got, got_last, limit, unit_places, out_f, lse, grad_got, grad_got_last
    )
    back, back_last = exchange(5, -1, grad_sent, grad_sent_last)
    last_parts = back[:, 192:256, :].astype(f32).reshape(2, half, HEAD_DIM, 256)
    last_sums = jnp.sum(last_parts, 1).astype(bf)
    grad_query = jnp.concatenate(
        [back[:, 0:64].reshape(cut, count), jnp.concatenate([back_last[0], back_last[1]], 1)], 0
    )
    grad_key = jnp.concatenate(
        [
            back[:, 64:128].reshape(cut, count),
            jnp.concatenate([last_sums[0, :, :128], last_sums[1, :, :128]], 1),
        ],
        0,
    )
    grad_value = jnp.concatenate(
        [
            back[:, 128:192].reshape(cut, count),
            jnp.concatenate([last_sums[0, :, 128:], last_sums[1, :, 128:]], 1),
        ],
        0,
    )
    grad_bias_query = jnp.sum(grad_query, 1, dtype=f32)
    grad_bias_value = jnp.sum(grad_value, 1, dtype=f32)
    grad_joined = jnp.concatenate([grad_query, grad_key, grad_value], 0)
    (joined_pair,) = share(6, grad_joined)
    grad_mat_qkv = both(own_columns(firsts), joined_pair, (0, 1), (0, 2))
    grad_first = contract(grad_joined, mat_qkv, 0, 1)
    grad_rows_norm, grad_gain_one, grad_shift_one = norm_one_pull(grad_first)
    tokens_grad = (grad_middle + grad_rows_norm).astype(bf).reshape(micro, 1, rows_here, width)

    small_grads = jnp.concatenate(
        [
            item.reshape(2, -1)
            for item in (
                grad_gain_one,
                grad_shift_one,
                grad_bias_query,
                grad_bias_value,
                grad_bias_out,
                grad_gain_two,
                grad_shift_two,
                grad_bias_proj,
                grad_bias_fc,
            )
        ],
        1,
    )
    lanes = 128
    rows = -(-small_grads.shape[1] // (8 * lanes)) * 8
    small_rows = jnp.pad(small_grads, ((0, 0), (0, rows * lanes - small_grads.shape[1])))
    sum_fc, sum_rest, sum_proj, small_own = sum_grads(
        7,
        grad_mat_fc,
        jnp.concatenate([grad_mat_qkv, grad_mat_out], 1),
        grad_mat_proj,
        small_rows.reshape(2, rows, lanes),
    )
    small_own = small_own.reshape(-1)
    vec = [small_own[i * part : (i + 1) * part] for i in range(8)]
    vec.append(small_own[8 * part : 8 * part + hidden_width // 2])
    return (
        result,
        tokens_grad,
        vec[0],
        vec[1],
        sum_rest[:, : 3 * width].astype(f32),
        vec[2],
        vec[3],
        sum_rest[:, 3 * width :].astype(f32),
        vec[4],
        vec[5],
        vec[6],
        sum_fc.astype(f32),
        vec[8],
        sum_proj.astype(f32),
        vec[7],
    )


def specs():
    wide = P(None, "group", "replica", None)
    row, mat = P("group"), P("group", None)
    in_specs = (wide, wide, P(None, "group", "replica"), P(None, "group"))
    in_specs += (row, row, mat, row, row, mat, row, row, row, mat, row, mat, row)
    out_specs = (wide, wide, row, row, mat, row, row, mat, row, row, row, mat, row, mat, row)
    return in_specs, out_specs


def solution(mesh):
    by_heads = mesh.shape["replica"] == HEADS - 1 and mesh.shape["group"] == 2
    in_specs, out_specs = specs()
    return jax.shard_map(
        per_device_heads if by_heads else per_device_gather,
        mesh=mesh,
        in_specs=in_specs,
        out_specs=out_specs,
        check_vma=False,
    )
```

```python
import functools

import jax
import jax.numpy as jnp
from jax import lax
from jax.experimental import pallas as pl
from jax.experimental.pallas import tpu as pltpu
from jax.sharding import PartitionSpec as P

HEADS = 17
HEAD_DIM = 64
MESH = pl.DeviceIdType.MESH


def for_sending(array):

    def short(part):
        return part.astype(jnp.bfloat16) if part.dtype == jnp.float32 else part

    return jax.tree.map(short, array)


def norm_rows(values, gain, shift):
    center = values - jnp.mean(values, -1, keepdims=True)
    spread = jnp.mean(center * center, -1, keepdims=True)
    return center * lax.rsqrt(spread + 1e-05) * gain + shift


def gelu_tanh(values):
    return jax.nn.gelu(values, approximate=True)


def inner_rows(left, right):
    return lax.dot_general(
        left, right, (((0,), (0,)), ((), ())), preferred_element_type=jnp.float32
    )


def times_transposed(left, right):
    return lax.dot_general(
        left, right, (((1,), (1,)), ((), ())), preferred_element_type=jnp.float32
    )


def masked_scores(queries, keys, query_place, key_place, prefix_len, scale):
    scores = jnp.einsum("qhe,khe->hqk", queries, keys, preferred_element_type=jnp.float32) * scale
    allowed = (key_place[None, :] <= query_place[:, None]) | (key_place[None, :] < prefix_len)
    return jnp.where(allowed[None], scores, -1e30)


def reduce_grads(terms):
    owned = jax.tree.map(
        lambda part: part.astype(jnp.float32),
        lax.psum_scatter(for_sending(terms), "group", scatter_dimension=0, tiled=True),
    )
    return jax.tree.map(
        lambda part: part.astype(jnp.float32), lax.psum(for_sending(owned), "replica")
    )


def per_device_gather(
    tokens,
    out_grad,
    positions,
    prefix,
    ln1_gain,
    ln1_bias,
    w_qkv,
    b_query,
    b_value,
    w_attn_out,
    b_attn_out,
    ln2_gain,
    ln2_bias,
    w_fc,
    b_fc,
    w_proj,
    b_proj,
):
    shards = (
        ln1_gain,
        ln1_bias,
        w_qkv,
        b_query,
        b_value,
        w_attn_out,
        b_attn_out,
        ln2_gain,
        ln2_bias,
        w_fc,
        b_fc,
        w_proj,
        b_proj,
    )
    micro = tokens.shape[0]
    rows_here = tokens.shape[2]
    width = tokens.shape[3]
    scale = HEAD_DIM ** (-0.5)
    head_shape = (rows_here, HEADS, HEAD_DIM)
    all_places = lax.all_gather(positions, "replica", axis=2, tiled=True)
    outputs_list = []
    grads_list = []
    kept = None
    owned = None
    for step in range(micro):
        full = (
            lax.all_gather(shards[0], "group", axis=0, tiled=True),
            lax.all_gather(shards[1], "group", axis=0, tiled=True),
            lax.all_gather(shards[2], "group", axis=0, tiled=True),
            lax.all_gather(shards[3], "group", axis=0, tiled=True),
            lax.all_gather(shards[4], "group", axis=0, tiled=True),
            lax.all_gather(shards[5], "group", axis=0, tiled=True),
            lax.all_gather(shards[6], "group", axis=0, tiled=True),
            lax.all_gather(shards[7], "group", axis=0, tiled=True),
            lax.all_gather(shards[8], "group", axis=0, tiled=True),
            lax.all_gather(shards[9], "group", axis=0, tiled=True),
            lax.all_gather(shards[10], "group", axis=0, tiled=True),
            lax.all_gather(shards[11], "group", axis=0, tiled=True),
            lax.all_gather(shards[12], "group", axis=0, tiled=True),
        )
        (
            gain_one,
            shift_one,
            mat_qkv,
            bias_query,
            bias_value,
            mat_out,
            bias_out,
            gain_two,
            shift_two,
            mat_fc,
            bias_fc,
            mat_proj,
            bias_proj,
        ) = full
        gain_one = gain_one.astype(jnp.float32)
        shift_one = shift_one.astype(jnp.float32)
        bias_query = bias_query.astype(jnp.float32)
        bias_value = bias_value.astype(jnp.float32)
        bias_out = bias_out.astype(jnp.float32)
        gain_two = gain_two.astype(jnp.float32)
        shift_two = shift_two.astype(jnp.float32)
        bias_fc = bias_fc.astype(jnp.float32)
        bias_proj = bias_proj.astype(jnp.float32)
        rows_in = tokens[step, 0].astype(jnp.float32)
        query_place = positions[step, 0]
        key_place = all_places[step, 0]
        prefix_len = prefix[step, 0]
        normed_one, norm_one_pull = jax.vjp(norm_rows, rows_in, gain_one, shift_one)
        first = normed_one.astype(jnp.bfloat16)
        joined = jnp.dot(first, mat_qkv, preferred_element_type=jnp.float32)
        queries = (joined[:, :width] + bias_query).astype(jnp.bfloat16)
        keys = joined[:, width : 2 * width].astype(jnp.bfloat16)
        values = (joined[:, 2 * width :] + bias_value).astype(jnp.bfloat16)
        key_all, value_all = (
            lax.all_gather(keys, "replica", axis=0, tiled=True),
            lax.all_gather(values, "replica", axis=0, tiled=True),
        )
        length = key_all.shape[0]
        block = min(512, length)
        nblocks = length // block
        query_heads = queries.reshape(head_shape)
        key_blocks = key_all.reshape(nblocks, block, HEADS, HEAD_DIM)
        value_blocks = value_all.reshape(nblocks, block, HEADS, HEAD_DIM)
        place_blocks = key_place.reshape(nblocks, block)

        def attend_step(carry, blockargs):
            highest, total, summed = carry
            key_part, value_part, place_part = blockargs
            scores = masked_scores(
                query_heads, key_part, query_place, place_part, prefix_len, scale
            )
            new_high = jnp.maximum(highest, jnp.max(scores, -1))
            factor = jnp.exp(highest - new_high)
            expo = jnp.exp(scores - new_high[..., None])
            total = total * factor + jnp.sum(expo, -1)
            summed = summed * jnp.transpose(factor)[..., None] + jnp.einsum(
                "hqk,khe->qhe",
                expo.astype(jnp.bfloat16),
                value_part,
                preferred_element_type=jnp.float32,
            )
            return ((new_high, total, summed), None)

        start_carry = (
            jnp.full((HEADS, rows_here), -1e30, jnp.float32),
            jnp.zeros((HEADS, rows_here), jnp.float32),
            jnp.zeros(head_shape, jnp.float32),
        )
        (highest, total, summed), _ = lax.scan(
            attend_step, start_carry, (key_blocks, value_blocks, place_blocks)
        )
        log_total = highest + jnp.log(total)
        attended_f = summed / jnp.transpose(total)[..., None]
        attended = attended_f.reshape(rows_here, width).astype(jnp.bfloat16)
        middle = rows_in + jnp.dot(attended, mat_out, preferred_element_type=jnp.float32) + bias_out
        normed_two, norm_two_pull = jax.vjp(norm_rows, middle, gain_two, shift_two)
        second = normed_two.astype(jnp.bfloat16)
        hidden_in = jnp.dot(second, mat_fc, preferred_element_type=jnp.float32) + bias_fc
        hidden_f, gelu_pull = jax.vjp(gelu_tanh, hidden_in)
        hidden = hidden_f.astype(jnp.bfloat16)
        output_rows = (
            middle + jnp.dot(hidden, mat_proj, preferred_element_type=jnp.float32) + bias_proj
        )
        outputs_list.append(output_rows.astype(jnp.bfloat16))
        grad_top = out_grad[step, 0].astype(jnp.float32)
        grad_low = out_grad[step, 0]
        grad_bias_proj = jnp.sum(grad_top, 0)
        grad_mat_proj = inner_rows(hidden, grad_low)
        grad_hidden = times_transposed(grad_low, mat_proj)
        (grad_hidden_in,) = gelu_pull(grad_hidden)
        grad_hidden_in = grad_hidden_in.astype(jnp.bfloat16)
        grad_bias_fc = jnp.sum(grad_hidden_in, 0, dtype=jnp.float32)
        grad_mat_fc = inner_rows(second, grad_hidden_in)
        grad_second = times_transposed(grad_hidden_in, mat_fc)
        grad_middle_norm, grad_gain_two, grad_shift_two = norm_two_pull(grad_second)
        grad_middle = grad_top + grad_middle_norm
        grad_bias_out = jnp.sum(grad_middle, 0)
        grad_branch = grad_middle.astype(jnp.bfloat16)
        grad_mat_out = inner_rows(attended, grad_branch)
        grad_attended = times_transposed(grad_branch, mat_out).astype(jnp.bfloat16)
        grad_heads = grad_attended.reshape(head_shape)
        delta = jnp.transpose(jnp.sum(grad_heads.astype(jnp.float32) * attended_f, -1))

        def score_grads(
            query_part, grad_part, key_part, value_part, qplace, kplace, lse_part, delta_part
        ):
            scores = masked_scores(query_part, key_part, qplace, kplace, prefix_len, scale)
            probs = jnp.exp(scores - lse_part[..., None])
            grad_probs = jnp.einsum(
                "qhe,khe->hqk", grad_part, value_part, preferred_element_type=jnp.float32
            )
            grad_scores = (probs * (grad_probs - delta_part[..., None])).astype(jnp.bfloat16)
            return (probs.astype(jnp.bfloat16), grad_scores)

        def grad_step(summed, blockargs):
            key_part, value_part, place_part = blockargs
            probs, grad_scores = score_grads(
                query_heads,
                grad_heads,
                key_part,
                value_part,
                query_place,
                place_part,
                log_total,
                delta,
            )
            summed = summed + jnp.einsum(
                "hqk,khe->qhe", grad_scores, key_part, preferred_element_type=jnp.float32
            )
            key_grad = jnp.einsum(
                "hqk,qhe->khe", grad_scores, query_heads, preferred_element_type=jnp.float32
            )
            value_grad = jnp.einsum(
                "hqk,qhe->khe", probs, grad_heads, preferred_element_type=jnp.float32
            )
            return (summed, (key_grad, value_grad))

        grad_query, (key_grads, value_grads) = lax.scan(
            grad_step, jnp.zeros(head_shape, jnp.float32), (key_blocks, value_blocks, place_blocks)
        )
        grad_key, grad_value = (
            lax.psum_scatter(
                key_grads.reshape(length, width).astype(jnp.bfloat16),
                "replica",
                scatter_dimension=0,
                tiled=True,
            ).astype(jnp.float32),
            lax.psum_scatter(
                value_grads.reshape(length, width).astype(jnp.bfloat16),
                "replica",
                scatter_dimension=0,
                tiled=True,
            ).astype(jnp.float32),
        )
        grad_query = (grad_query.reshape(rows_here, width) * scale).astype(jnp.bfloat16)
        grad_key = (grad_key * scale).astype(jnp.bfloat16)
        grad_value = grad_value.astype(jnp.bfloat16)
        grad_bias_query = jnp.sum(grad_query, 0, dtype=jnp.float32)
        grad_bias_value = jnp.sum(grad_value, 0, dtype=jnp.float32)
        grad_joined = jnp.concatenate([grad_query, grad_key, grad_value], 1)
        grad_mat_qkv = inner_rows(first, grad_joined)
        grad_first = times_transposed(grad_joined, mat_qkv)
        grad_rows_norm, grad_gain_one, grad_shift_one = norm_one_pull(grad_first)
        grads_list.append((grad_middle + grad_rows_norm).astype(jnp.bfloat16))
        terms = (
            grad_gain_one,
            grad_shift_one,
            grad_mat_qkv,
            grad_bias_query,
            grad_bias_value,
            grad_mat_out,
            grad_bias_out,
            grad_gain_two,
            grad_shift_two,
            grad_mat_fc,
            grad_bias_fc,
            grad_mat_proj,
            grad_bias_proj,
        )
        kept = (
            terms
            if kept is None
            else tuple((first_term + second_term for first_term, second_term in zip(kept, terms)))
        )
    owned = reduce_grads(kept)
    result = jnp.stack(outputs_list).reshape(micro, 1, rows_here, width)
    tokens_grad = jnp.stack(grads_list).reshape(micro, 1, rows_here, width)
    return (result, tokens_grad) + tuple(owned)


def contract(left, right, left_dim, right_dim):
    return lax.dot_general(
        left, right, (((left_dim,), (right_dim,)), ((), ())), preferred_element_type=jnp.float32
    )


def greet(peers, here, group_too):
    barrier = pltpu.get_barrier_semaphore()

    def one(step, carry):
        peer = lax.rem(here + step, peers)
        pl.semaphore_signal(barrier, inc=1, device_id={"replica": peer}, device_id_type=MESH)
        return carry

    lax.fori_loop(1, peers, one, 0)
    if group_too:
        other = 1 - lax.axis_index("group")
        pl.semaphore_signal(barrier, inc=1, device_id={"group": other}, device_id_type=MESH)
    pl.semaphore_wait(barrier, peers - 1 + (1 if group_too else 0))


def halves(ref, mode, which):
    if mode == "whole":
        return ref
    if mode == "rows":
        size = ref.shape[0] // 2
        return ref.at[pl.ds(pl.multiple_of(which * size, 16), size)]
    size = ref.shape[1] // 2
    return ref.at[:, pl.ds(pl.multiple_of(which * size, 128), size)]


def half_shape(array, mode):
    rows, columns = array.shape
    return {"whole": (rows, columns), "rows": (rows // 2, columns), "columns": (rows, columns // 2)}[mode]


def exchange_body(direction, with_places, modes, *refs):
    refs = list(refs)
    nweights = len(modes)
    chunk, last = refs.pop(0), refs.pop(0)
    places = refs.pop(0) if with_places else None
    weights = [refs.pop(0) for _ in range(nweights)]
    chunk_out, last_out = refs.pop(0), refs.pop(0)
    places_out = refs.pop(0) if with_places else None
    weights_out = [refs.pop(0) for _ in range(nweights)]
    send, recv, last_send, last_recv, own = (refs.pop(0) for _ in range(5))
    if with_places:
        place_send, place_recv = refs.pop(0), refs.pop(0)
    if nweights:
        weight_send, weight_recv, weight_own = (refs.pop(0) for _ in range(3))
        bounce = [refs.pop(0) for _ in range(nweights)]
    peers = chunk.shape[0]
    here = lax.axis_index("replica")
    group = lax.axis_index("group")
    greet(peers, here, nweights > 0)
    loads, copies = [], []
    for i in range(nweights):
        copy = pltpu.make_async_remote_copy(
            halves(weights[i], modes[i], 1 - group),
            weights_out[i].at[group],
            weight_send.at[i],
            weight_recv.at[i],
            device_id={"group": 1 - group},
            device_id_type=MESH,
        )
        copy.start()
        copies.append(copy)
        load = pltpu.make_async_copy(
            halves(weights[i], modes[i], group), bounce[i], weight_own.at[i]
        )
        load.start()
        loads.append(load)
    for slot in range(2):
        half = peers // 2
        target = lax.rem(here + direction + peers, half) + half * slot
        copy = pltpu.make_async_remote_copy(
            last.at[slot],
            last_out.at[here // half],
            last_send.at[slot],
            last_recv.at[here // half],
            device_id={"replica": target},
            device_id_type=MESH,
        )
        copy.start()
        copies.append(
            (
                copy,
                pltpu.make_async_remote_copy(
                    last.at[slot],
                    last_out.at[slot],
                    last_send.at[slot],
                    last_recv.at[slot],
                    device_id={"replica": target},
                    device_id_type=MESH,
                ),
            )
        )
    for step in range(1, peers):
        peer = lax.rem(here + step, peers)
        copy = pltpu.make_async_remote_copy(
            chunk.at[peer],
            chunk_out.at[here],
            send.at[step],
            recv.at[step],
            device_id={"replica": peer},
            device_id_type=MESH,
        )
        copy.start()
        copies.append(copy)
        if with_places:
            copy = pltpu.make_async_remote_copy(
                places,
                places_out.at[here],
                place_send.at[step],
                place_recv.at[step],
                device_id={"replica": peer},
                device_id_type=MESH,
            )
            copy.start()
            copies.append(copy)
    owns = [pltpu.make_async_copy(chunk.at[here], chunk_out.at[here], own.at[0])]
    if with_places:
        owns.append(pltpu.make_async_copy(places, places_out.at[here], own.at[1]))
    for copy in owns:
        copy.start()
    stores = []
    for i, load in enumerate(loads):
        load.wait()
        store = pltpu.make_async_copy(bounce[i], weights_out[i].at[group], weight_own.at[i])
        store.start()
        stores.append(store)
    for copy in stores + owns:
        copy.wait()
    for copy in copies:
        if isinstance(copy, tuple):
            copy[0].wait_send()
            copy[1].wait_recv()
        else:
            copy.wait()


def exchange(ident, direction, chunk, last, places=None, shares=()):
    peers = chunk.shape[0]
    weights = [array for array, _ in shares]
    modes = [mode for _, mode in shares]
    any_spec = pl.BlockSpec(memory_space=pl.ANY)
    with_places = places is not None
    args = [chunk, last] + ([places] if with_places else []) + list(weights)
    shapes = [(chunk.shape, chunk.dtype), (last.shape, last.dtype)]
    if with_places:
        shapes.append(((peers,) + places.shape, places.dtype))
    shapes += [((2,) + half_shape(*item), item[0].dtype) for item in shares]
    dma = pltpu.SemaphoreType.DMA
    scratch = [dma((peers,)), dma((peers,)), dma((2,)), dma((2,)), dma((2,))]
    if with_places:
        scratch += [dma((peers,)), dma((peers,))]
    if weights:
        count = len(weights)
        scratch += [dma((count,)), dma((count,)), dma((count,))]
        scratch += [pltpu.VMEM(half_shape(*item), item[0].dtype) for item in shares]
    return pl.pallas_call(
        functools.partial(exchange_body, direction, with_places, modes),
        out_shape=[jax.ShapeDtypeStruct(*shape) for shape in shapes],
        in_specs=[any_spec] * len(args),
        out_specs=[any_spec] * len(shapes),
        scratch_shapes=scratch,
        compiler_params=pltpu.CompilerParams(collective_id=ident, has_side_effects=True),
        name=f"exchange{ident}",
    )(*args)


def share_body(count, *refs):
    sources, results = refs[:count], refs[count : 2 * count]
    send, recv, own = refs[2 * count : 2 * count + 3]
    bounce = refs[2 * count + 3 :]
    group = lax.axis_index("group")
    barrier = pltpu.get_barrier_semaphore()
    pl.semaphore_signal(barrier, inc=1, device_id={"group": 1 - group}, device_id_type=MESH)
    pl.semaphore_wait(barrier, 1)
    copies, loads, stores = [], [], []
    for i in range(count):
        copy = pltpu.make_async_remote_copy(
            sources[i],
            results[i].at[group],
            send.at[i],
            recv.at[i],
            device_id={"group": 1 - group},
            device_id_type=MESH,
        )
        copy.start()
        copies.append(copy)
        load = pltpu.make_async_copy(sources[i], bounce[i], own.at[i])
        load.start()
        loads.append(load)
    for i in range(count):
        loads[i].wait()
        store = pltpu.make_async_copy(bounce[i], results[i].at[group], own.at[i])
        store.start()
        stores.append(store)
    for copy in stores + copies:
        copy.wait()


def share(ident, *arrays):
    count = len(arrays)
    any_spec = pl.BlockSpec(memory_space=pl.ANY)
    dma = pltpu.SemaphoreType.DMA
    return pl.pallas_call(
        functools.partial(share_body, count),
        out_shape=[jax.ShapeDtypeStruct((2,) + a.shape, a.dtype) for a in arrays],
        in_specs=[any_spec] * count,
        out_specs=[any_spec] * count,
        scratch_shapes=[dma((count,)), dma((count,)), dma((count,))]
        + [pltpu.VMEM(a.shape, a.dtype) for a in arrays],
        compiler_params=pltpu.CompilerParams(collective_id=ident, has_side_effects=True),
        name=f"share{ident}",
    )(*arrays)


BLOCK = 256


def unpack_units(got, last, rows_at, query_out):
    peers = got.shape[0]
    half = BLOCK // 128
    for m in range(2):
        for s in range(peers):
            query_out[m * (peers // half) + s // half, :, (s % half) * 128 : (s % half + 1) * 128] = got[
                s, rows_at : rows_at + 64, m * 128 : (m + 1) * 128
            ]
    extra = 2 * (peers // half)
    for j in range(2):
        query_out[extra, :, j * 128 : (j + 1) * 128] = last[j]


def unit_source(got, u, s, first):
    if u < 2:
        return got[s, first : first + 64, u * 128 : (u + 1) * 128]
    at = 0 if first == 64 else 128
    return got[s, 192:256, at : at + 128]


def attend_body(got, last, limit, places, sent, last_sent, out_f, lse, keys, values, queries, outs):
    peers = got.shape[0]
    nblocks = queries.shape[0]
    per_unit = (nblocks - 1) // 2
    unpack_units(got, last, 0, queries)
    for u in range(3):
        for s in range(peers):
            span = slice(s * 128, (s + 1) * 128)
            keys[u, span, :] = unit_source(got, u, s, 64).T
            values[u, :, span] = unit_source(got, u, s, 128)

    def block(b, carry):
        u = b // per_unit
        scores = jnp.dot(keys[u], queries[b], preferred_element_type=jnp.float32)
        place = places[u]
        place = jnp.concatenate([place, place], axis=1)
        scores = jnp.where(place < limit[b], scores, -1e30)
        high = jnp.max(scores, axis=0, keepdims=True)
        expo = jnp.exp(scores - high)
        total = jnp.sum(expo, axis=0, keepdims=True)
        summed = jnp.dot(values[u], expo.astype(jnp.bfloat16), preferred_element_type=jnp.float32)
        result = summed / total
        out_f[b] = result
        outs[b] = result.astype(jnp.bfloat16)
        lse[b] = high + jnp.log(total)
        return carry

    lax.fori_loop(0, nblocks, block, 0)
    half = BLOCK // 128
    for m in range(2):
        for s in range(peers):
            sent[s, :, m * 128 : (m + 1) * 128] = outs[
                m * per_unit + s // half, :, (s % half) * 128 : (s % half + 1) * 128
            ]
    for j in range(2):
        last_sent[j] = outs[nblocks - 1, :, j * 128 : (j + 1) * 128]


def attend(got, last, limit, places):
    peers = got.shape[0]
    nblocks = limit.shape[0]
    length = places.shape[1]
    bf, f32 = jnp.bfloat16, jnp.float32
    return pl.pallas_call(
        attend_body,
        out_shape=[
            jax.ShapeDtypeStruct((peers, 64, 256), bf),
            jax.ShapeDtypeStruct((2, 64, 128), bf),
            jax.ShapeDtypeStruct((nblocks, 64, BLOCK), f32),
            jax.ShapeDtypeStruct((nblocks, 1, BLOCK), f32),
        ],
        scratch_shapes=[
            pltpu.VMEM((3, length, 64), bf),
            pltpu.VMEM((3, 64, length), bf),
            pltpu.VMEM((nblocks, 64, BLOCK), bf),
            pltpu.VMEM((nblocks, 64, BLOCK), bf),
        ],
        compiler_params=pltpu.CompilerParams(vmem_limit_bytes=56 << 20),
        name="attend",
    )(got, last, limit, places)


def attend_grad_body(
    got,
    last,
    limit,
    places,
    out_f,
    lse,
    grad_got,
    grad_last,
    sent,
    last_sent,
    keys,
    keys_t,
    values,
    queries,
    grads,
    queries_n,
    grads_n,
    dqs,
    dk,
    dv,
):
    peers = got.shape[0]
    nblocks = queries.shape[0]
    per_unit = (nblocks - 1) // 2
    unpack_units(got, last, 0, queries)
    unpack_units(grad_got, grad_last, 0, grads)
    for u in range(3):
        for s in range(peers):
            span = slice(s * 128, (s + 1) * 128)
            part = unit_source(got, u, s, 64)
            keys[u, span, :] = part.T
            keys_t[u, :, span] = part
            values[u, span, :] = unit_source(got, u, s, 128).T
    for b in range(nblocks):
        queries_n[b] = queries[b].T
        grads_n[b] = grads[b].T
    dk[...] = jnp.zeros_like(dk)
    dv[...] = jnp.zeros_like(dv)

    def block(b, carry):
        u = b // per_unit
        grad = grads[b]
        delta = jnp.sum(grad.astype(jnp.float32) * out_f[b], axis=0, keepdims=True)
        scores = jnp.dot(keys[u], queries[b], preferred_element_type=jnp.float32)
        place = places[u]
        place = jnp.concatenate([place, place], axis=1)
        scores = jnp.where(place < limit[b], scores, -1e30)
        probs = jnp.exp(scores - lse[b])
        grad_probs = jnp.dot(values[u], grad, preferred_element_type=jnp.float32)
        grad_scores = (probs * (grad_probs - delta)).astype(jnp.bfloat16)
        dqs[b] = jnp.dot(keys_t[u], grad_scores, preferred_element_type=jnp.float32)
        dk[u] += jnp.dot(grad_scores, queries_n[b], preferred_element_type=jnp.float32)
        dv[u] += jnp.dot(probs.astype(jnp.bfloat16), grads_n[b], preferred_element_type=jnp.float32)
        return carry

    lax.fori_loop(0, nblocks, block, 0)
    half = BLOCK // 128
    scale = HEAD_DIM ** (-0.5)
    for m in range(2):
        for s in range(peers):
            at = slice(m * 128, (m + 1) * 128)
            span = slice(s * 128, (s + 1) * 128)
            dq = dqs[m * per_unit + s // half, :, (s % half) * 128 : (s % half + 1) * 128]
            sent[s, 0:64, at] = (dq * scale).astype(jnp.bfloat16)
            sent[s, 64:128, at] = dk[m, span, :].T.astype(jnp.bfloat16)
            sent[s, 128:192, at] = dv[m, span, :].T.astype(jnp.bfloat16)
    for s in range(peers):
        span = slice(s * 128, (s + 1) * 128)
        sent[s, 192:256, 0:128] = dk[2, span, :].T.astype(jnp.bfloat16)
        sent[s, 192:256, 128:256] = dv[2, span, :].T.astype(jnp.bfloat16)
    for j in range(2):
        last_sent[j] = (dqs[nblocks - 1, :, j * 128 : (j + 1) * 128] * scale).astype(jnp.bfloat16)


def attend_grad(got, last, limit, places, out_f, lse, grad_got, grad_last):
    peers = got.shape[0]
    nblocks = limit.shape[0]
    length = places.shape[1]
    bf, f32 = jnp.bfloat16, jnp.float32
    return pl.pallas_call(
        attend_grad_body,
        out_shape=[
            jax.ShapeDtypeStruct((peers, 256, 256), bf),
            jax.ShapeDtypeStruct((2, 64, 128), bf),
        ],
        scratch_shapes=[
            pltpu.VMEM((3, length, 64), bf),
            pltpu.VMEM((3, 64, length), bf),
            pltpu.VMEM((3, length, 64), bf),
            pltpu.VMEM((nblocks, 64, BLOCK), bf),
            pltpu.VMEM((nblocks, 64, BLOCK), bf),
            pltpu.VMEM((nblocks, BLOCK, 64), bf),
            pltpu.VMEM((nblocks, BLOCK, 64), bf),
            pltpu.VMEM((nblocks, 64, BLOCK), f32),
            pltpu.VMEM((3, length, 64), f32),
            pltpu.VMEM((3, length, 64), f32),
        ],
        compiler_params=pltpu.CompilerParams(vmem_limit_bytes=60 << 20),
        name="attend_grad",
    )(got, last, limit, places, out_f, lse, grad_got, grad_last)


ROWS = 272
PART = 80
PADDED = 4 * PART
PROJ, FC, OUT, QKV = range(4)
TILES = {PROJ: (9, 8), FC: (9, 8), OUT: (5,), QKV: (7, 6)}


def chunk_plan():
    plan = []
    for array in (PROJ, FC, OUT, QKV):
        start = 0
        for tiles in TILES[array]:
            plan.append((array, tiles * 128, start))
            start += tiles * 128
    return plan


def piece(ref, item, first, second):
    array, width, start = item
    if array == PROJ:
        row = first * (2 * ROWS) + second * ROWS
        return ref.at[pl.ds(pl.multiple_of(row, 16), ROWS), pl.ds(start, width)]
    column = second * (sum(TILES[array]) * 128) + start
    return ref.at[
        pl.ds(pl.multiple_of(first * ROWS, 16), ROWS), pl.ds(pl.multiple_of(column, 128), width)
    ]


def by_rows(rows, fn):
    def one(i, carry):
        fn(pl.multiple_of(i * 16, 16))
        return carry

    lax.fori_loop(0, rows // 16, one, 0)


class Summer:
    def __init__(self, plan, sources, results, own, came, second_in, quarter, parts, gathered, sems):
        self.plan, self.sources, self.results = plan, sources, results
        self.own, self.came, self.second_in = own, came, second_in
        self.quarter, self.parts, self.gathered = quarter, parts, gathered
        self.load_sem, self.store_sem = sems[0], sems[1]
        self.pairs = [tuple(sems[2 + 2 * i : 4 + 2 * i]) for i in range(6)]
        here, group = lax.axis_index("replica"), lax.axis_index("group")
        bit_x, bit_y = here % 2, (here // 2) % 2
        self.here, self.place = here, here // 4
        self.one = bit_x + group * (bit_y - bit_x)
        self.two = bit_x + bit_y - self.one
        self.peer_one = here + (1 + group) * (1 - 2 * self.one)
        self.peer_two = here + (2 - group) * (1 - 2 * self.two)

    def copy(self, stage, at, source, target, peer):
        send, recv = self.pairs[stage]
        return pltpu.make_async_remote_copy(
            source,
            target,
            send.at[at],
            recv.at[at],
            device_id={"replica": peer},
            device_id_type=MESH,
        )

    def z_peer(self, k):
        return lax.rem(self.here + 4 * k, 16)

    def block(self, place):
        return pl.ds(pl.multiple_of(place * PART, 16), PART)

    def load(self, c, j):
        item = self.plan[c]
        source = piece(self.sources[item[0]], item, self.one, j)
        return pltpu.make_async_copy(source, self.own[c].at[j], self.load_sem.at[c, j])

    def first(self, c, j):
        item = self.plan[c]
        source = piece(self.sources[item[0]], item, 1 - self.one, j)
        return self.copy(0, (c, j), source, self.came[c].at[j], self.peer_one)

    def second(self, c):
        return self.copy(1, (c,), self.own[c].at[1 - self.two], self.second_in[c], self.peer_two)

    def spread(self, c, k):
        source = self.quarter[c].at[self.block(lax.rem(self.place + k, 4))]
        return self.copy(2, (c, k - 1), source, self.parts[c].at[k - 1], self.z_peer(k))

    def gather(self, c, k):
        block = self.gathered[c].at[self.block(self.place)]
        return self.copy(3, (c, k - 1), block, block, self.z_peer(k))

    def result(self, c, other):
        item = self.plan[c]
        second = self.two + other * (1 - 2 * self.two)
        return piece(self.results[item[0]], item, self.one, second)

    def cross(self, c):
        return self.copy(
            4, (c,), self.gathered[c].at[pl.ds(0, ROWS)], self.result(c, 0), self.peer_two
        )

    def crossed(self, c):
        return self.copy(
            4, (c,), self.gathered[c].at[pl.ds(0, ROWS)], self.result(c, 1), self.peer_two
        )

    def final(self, c, other):
        source = self.result(c, 1) if other else self.gathered[c].at[pl.ds(0, ROWS)]
        return self.copy(5, (c, other), source, self.result(c, other), self.peer_one)

    def finalled(self, c, other):
        item = self.plan[c]
        second = self.two + other * (1 - 2 * self.two)
        target = piece(self.results[item[0]], item, 1 - self.one, second)
        source = self.result(c, 1) if other else self.gathered[c].at[pl.ds(0, ROWS)]
        return self.copy(5, (c, other), source, target, self.peer_one)

    def store(self, c):
        return pltpu.make_async_copy(
            self.gathered[c].at[pl.ds(0, ROWS)], self.result(c, 0), self.store_sem.at[c]
        )

    def begin(self, c):
        for j in range(2):
            self.first(c, j).start()
            self.load(c, j).start()
        width = self.quarter[c].shape[1]
        self.quarter[c][ROWS:, :] = jnp.zeros((PADDED - ROWS, width), jnp.bfloat16)

    def stage_one(self, c):
        for j in range(2):
            self.load(c, j).wait()
            self.first(c, j).wait_recv()
        away, own, came = 1 - self.two, self.own[c], self.came[c]

        def add(start):
            rows = pl.ds(start, 16)
            total = own[away, rows].astype(jnp.float32) + came[away, rows].astype(jnp.float32)
            own[away, rows] = total.astype(jnp.bfloat16)

        by_rows(ROWS, add)
        self.second(c).start()

    def stage_two(self, c):
        self.second(c).wait_recv()
        keep, own, came = self.two, self.own[c], self.came[c]

        def add(start):
            rows = pl.ds(start, 16)
            total = own[keep, rows].astype(jnp.float32) + came[keep, rows].astype(jnp.float32)
            total = total + self.second_in[c][rows].astype(jnp.float32)
            self.quarter[c][rows] = total.astype(jnp.bfloat16)

        by_rows(ROWS, add)
        for k in (1, 2, 3):
            self.spread(c, k).start()

    def stage_three(self, c):
        for k in (1, 2, 3):
            self.spread(c, k).wait_recv()

        def add(start):
            at = pl.ds(pl.multiple_of(self.place * PART + start, 16), 16)
            total = self.quarter[c][at].astype(jnp.float32)
            for k in range(3):
                total = total + self.parts[c][k, pl.ds(start, 16)].astype(jnp.float32)
            self.gathered[c][at] = total.astype(jnp.bfloat16)

        by_rows(PART, add)
        for k in (1, 2, 3):
            self.gather(c, k).start()

    def stage_four(self, c):
        for k in (1, 2, 3):
            self.spread(c, k).wait_send()
            self.gather(c, k).wait_recv()
        self.cross(c).start()
        self.final(c, 0).start()
        self.store(c).start()

    def stage_five(self, c):
        self.crossed(c).wait_recv()
        self.final(c, 1).start()

    def end(self, c):
        for j in range(2):
            self.finalled(c, j).wait_recv()
            self.first(c, j).wait_send()
            self.final(c, j).wait_send()
        self.second(c).wait_send()
        for k in (1, 2, 3):
            self.gather(c, k).wait_send()
        self.cross(c).wait_send()
        self.store(c).wait()

    def run(self, stage, c):
        steps = (self.stage_one, self.stage_two, self.stage_three, self.stage_four, self.stage_five)
        steps[stage](c)


def wavefront(chunks):
    order = []
    for tick in range(len(chunks) + 4):
        for stage in reversed(range(5)):
            if 0 <= tick - stage < len(chunks):
                order.append((stage, chunks[tick - stage]))
    return order


class SmallSum:
    def __init__(self, source, result, from_core, own, everyone, sems):
        self.source, self.result, self.from_core = source, result, from_core
        self.own, self.everyone = own, everyone
        (self.sp, self.rp, self.sa, self.ra, self.sb, self.rb) = sems
        self.here, self.group = lax.axis_index("replica"), lax.axis_index("group")
        self.peers = everyone.shape[0]

    def core_copy(self, source, target, send, recv):
        return pltpu.make_async_remote_copy(
            source,
            target,
            send,
            recv,
            device_id={"group": 1 - self.group},
            device_id_type=MESH,
        )

    def give(self):
        return self.core_copy(self.source.at[1 - self.group], self.from_core, self.sp, self.rp)

    def tell(self, step):
        return pltpu.make_async_remote_copy(
            self.own,
            self.everyone.at[self.here],
            self.sa.at[step],
            self.ra.at[step],
            device_id={"replica": lax.rem(self.here + step, self.peers)},
            device_id_type=MESH,
        )

    def back(self):
        return self.core_copy(
            self.result.at[self.group], self.result.at[self.group], self.sb, self.rb
        )

    def begin(self):
        self.give().start()

    def middle(self):
        self.give().wait()
        self.own[...] = self.source[self.group] + self.from_core[...]
        self.everyone[self.here] = self.own[...]
        for step in range(1, self.peers):
            self.tell(step).start()

    def finish(self):
        for step in range(1, self.peers):
            self.tell(step).wait()
        total = self.everyone[0]
        for i in range(1, self.peers):
            total = total + self.everyone[i]
        self.result[self.group] = total
        self.back().start()

    def end(self):
        self.back().wait()


def sum_grads_body(plan, *refs):
    nchunks = len(plan)
    sources, small, results, small_out = refs[0:4], refs[4], refs[5:9], refs[9]
    refs = list(refs[10:])
    buffers = [[refs.pop(0) for _ in range(nchunks)] for _ in range(6)]
    from_core, own_small, everyone = (refs.pop(0) for _ in range(3))
    summer = Summer(plan, sources, results, *buffers, refs[:14])
    smalls = SmallSum(small, small_out, from_core, own_small, everyone, refs[14:20])
    greet(everyone.shape[0], lax.axis_index("replica"), True)
    smalls.begin()
    for c in range(nchunks):
        summer.begin(c)
    smalls.middle()
    for stage, c in wavefront(range(nchunks)):
        summer.run(stage, c)
    smalls.finish()
    smalls.end()
    for c in range(nchunks):
        summer.end(c)


def sum_buffers(plan):
    bf = jnp.bfloat16
    shapes = ((2, ROWS), (2, ROWS), (ROWS,), (PADDED,), (3, PART), (PADDED,))
    return [pltpu.VMEM(shape + (item[1],), bf) for shape in shapes for item in plan]


def sum_sems(plan):
    dma = pltpu.SemaphoreType.DMA
    count = len(plan)
    pairs, triples, ones = dma((count, 2)), dma((count, 3)), dma((count,))
    stages = (pairs, ones, triples, triples, ones, pairs)
    return [pairs, ones] + [sem for stage in stages for sem in (stage, stage)]


def small_scratch(shape, peers):
    f32 = jnp.float32
    return [pltpu.VMEM(shape, f32), pltpu.VMEM(shape, f32), pltpu.VMEM((peers,) + shape, f32)]


def small_sems(peers):
    dma = pltpu.SemaphoreType.DMA
    return [dma, dma, dma((peers,)), dma((peers,)), dma, dma]


def sum_grads(ident, *arrays):
    *arrays, small = arrays
    plan = chunk_plan()
    peers = lax.axis_size("replica")
    bf, f32 = jnp.bfloat16, jnp.float32
    any_spec = pl.BlockSpec(memory_space=pl.ANY)
    vmem = pl.BlockSpec(memory_space=pltpu.VMEM)
    return pl.pallas_call(
        functools.partial(sum_grads_body, plan),
        out_shape=[jax.ShapeDtypeStruct(a.shape, bf) for a in arrays]
        + [jax.ShapeDtypeStruct(small.shape, f32)],
        in_specs=[any_spec] * 4 + [vmem],
        out_specs=[any_spec] * 4 + [vmem],
        scratch_shapes=sum_buffers(plan)
        + small_scratch(small.shape[1:], peers)
        + sum_sems(plan)
        + small_sems(peers),
        compiler_params=pltpu.CompilerParams(
            collective_id=ident, has_side_effects=True, vmem_limit_bytes=56 << 20
        ),
        name=f"sum_grads{ident}",
    )(*arrays, small)


def norm_unit(values):
    center = values - jnp.mean(values, -1, keepdims=True)
    spread = lax.rsqrt(jnp.mean(center * center, -1, keepdims=True) + 1e-05)
    return center * spread, spread


def norm_back(grad, unit, spread, gain):
    grad_unit = grad * gain
    slope = jnp.mean(grad_unit * unit, -1, keepdims=True)
    back = spread * (grad_unit - jnp.mean(grad_unit, -1, keepdims=True) - unit * slope)
    return back, jnp.sum(grad * unit, 0, keepdims=True), jnp.sum(grad, 0, keepdims=True)


def split_last(array):
    return jnp.stack([array[:, :128], array[:, 128:]])


def per_device_heads(
    tokens,
    out_grad,
    positions,
    prefix,
    ln1_gain,
    ln1_bias,
    w_qkv,
    b_query,
    b_value,
    w_attn_out,
    b_attn_out,
    ln2_gain,
    ln2_bias,
    w_fc,
    b_fc,
    w_proj,
    b_proj,
):
    bf, f32 = jnp.bfloat16, jnp.float32
    micro, _, rows_here, width = tokens.shape
    peers = lax.axis_size("replica")
    hidden_width = 2 * b_fc.shape[0]
    half = peers // 2
    count = micro * rows_here
    here = lax.axis_index("replica")
    scale = HEAD_DIM ** (-0.5)
    split = (peers * HEAD_DIM, width)

    vectors = (ln1_gain, ln1_bias, b_query, b_value, b_attn_out, ln2_gain, ln2_bias, b_proj, b_fc)
    shared = share(1, w_qkv, *(vector.reshape(1, -1) for vector in vectors))
    mat_qkv = shared[0].reshape(width, 3 * width)
    part = width // 2
    (
        gain_one,
        shift_one,
        bias_query,
        bias_value,
        bias_out,
        gain_two,
        shift_two,
        bias_proj,
        bias_fc,
    ) = (vector.reshape(1, -1).astype(f32) for vector in shared[1:])

    rows_in = tokens.reshape(count, width).astype(f32)
    unit_one, spread_one = norm_unit(rows_in)
    first = (unit_one * gain_one + shift_one).astype(bf)
    joined = contract(mat_qkv, first, 0, 1)
    bias_all = jnp.concatenate([bias_query, jnp.zeros_like(bias_query), bias_value], 1)
    joined = joined + bias_all.reshape(-1, 1)
    queries = ((joined[:width]).astype(bf).astype(f32) * scale).astype(bf)
    keys = joined[width : 2 * width].astype(bf)
    values = joined[2 * width :].astype(bf)
    cut = split[0]
    main = [part_[:cut].reshape(peers, HEAD_DIM, count) for part_ in (queries, keys, values)]
    key_last, value_last = keys[cut:], values[cut:]
    tails = jnp.stack(
        [
            jnp.concatenate(
                [key_last[:, m * 128 : (m + 1) * 128], value_last[:, m * 128 : (m + 1) * 128]], 1
            )
            for m in range(2)
        ]
    )
    tails = jnp.repeat(tails, half, axis=0)
    chunk = jnp.concatenate(main + [tails], axis=1)
    grad_low = out_grad.reshape(count, width)
    got, got_last, all_places, mat_out, mat_fc, mat_proj_t, firsts, grad_lows = exchange(
        2,
        1,
        chunk,
        split_last(queries[cut:]),
        positions.reshape(micro, rows_here),
        [(item, "whole") for item in (w_attn_out, w_fc, w_proj.T, first, grad_low)],
    )
    mat_out = mat_out.reshape(width, width)
    mat_fc = mat_fc.reshape(width, hidden_width)

    place_rows = jnp.transpose(all_places, (1, 0, 2)).reshape(micro, peers * rows_here)
    limits = jnp.maximum(place_rows + 1, prefix.reshape(micro, 1))
    mine = here // half
    at = lax.rem(here - 1 + peers, half)
    own_limits = lax.dynamic_index_in_dim(limits, mine, 0, False).reshape(peers, rows_here)
    own_limits = jnp.concatenate(
        [
            lax.dynamic_index_in_dim(own_limits, at, 0, True),
            lax.dynamic_index_in_dim(own_limits, at + half, 0, True),
        ],
        1,
    )
    limit = jnp.concatenate([limits.reshape(-1, BLOCK), own_limits], 0)[:, None, :]
    unit_places = jnp.concatenate(
        [place_rows, lax.dynamic_index_in_dim(place_rows, mine, 0, True)], 0
    )
    unit_places = jnp.broadcast_to(unit_places[:, :, None], unit_places.shape + (128,))

    sent, sent_last, out_f, lse = attend(got, got_last, limit, unit_places)
    heads_out, heads_last = exchange(3, -1, sent, sent_last)
    attended = jnp.concatenate(
        [heads_out.reshape(cut, count), jnp.concatenate([heads_last[0], heads_last[1]], 1)], 0
    )

    middle = rows_in + contract(attended, mat_out, 0, 0) + bias_out
    unit_two, spread_two = norm_unit(middle)
    second = (unit_two * gain_two + shift_two).astype(bf)
    hidden_in = jnp.dot(second, mat_fc, preferred_element_type=f32) + bias_fc
    hidden_f, gelu_pull = jax.vjp(gelu_tanh, hidden_in)
    hidden = hidden_f.astype(bf)
    output_rows = middle + bias_proj
    half_hidden = hidden_width // 2
    for core in range(2):
        own_hidden = hidden[:, core * half_hidden : (core + 1) * half_hidden]
        output_rows = output_rows + contract(own_hidden, mat_proj_t[core], 1, 1)
    result = output_rows.astype(bf).reshape(micro, 1, rows_here, width)

    grad_top = grad_low.astype(f32)
    grad_bias_proj = jnp.sum(grad_top, 0, keepdims=True)
    grad_hidden = jnp.concatenate([contract(grad_low, mat_proj_t[core], 1, 0) for core in range(2)], 1)
    (grad_hidden_in,) = gelu_pull(grad_hidden)
    grad_hidden_in = grad_hidden_in.astype(bf)
    grad_bias_fc = jnp.sum(grad_hidden_in, 0, keepdims=True, dtype=f32)
    grad_second = times_transposed(grad_hidden_in, mat_fc)
    grad_middle_norm, grad_gain_two, grad_shift_two = norm_back(
        grad_second, unit_two, spread_two, gain_two
    )
    grad_middle = grad_top + grad_middle_norm
    grad_bias_out = jnp.sum(grad_middle, 0, keepdims=True)
    grad_branch = grad_middle.astype(bf)
    grad_attended = contract(mat_out, grad_branch, 1, 1).astype(bf)

    grad_got, grad_got_last, hiddens, seconds, grad_ins, attendeds, branches = exchange(
        4,
        1,
        grad_attended[:cut].reshape(peers, HEAD_DIM, count),
        split_last(grad_attended[cut:]),
        None,
        [
            (hidden, "columns"),
            (second, "whole"),
            (grad_hidden_in, "whole"),
            (attended, "rows"),
            (grad_branch, "whole"),
        ],
    )
    group = lax.axis_index("group")

    def own_columns(pair):
        return lax.dynamic_slice_in_dim(pair, group * part, part, 2)

    def both(left, right, left_dims, right_dims):
        return lax.dot_general(
            left, right, ((left_dims, right_dims), ((), ())), preferred_element_type=f32
        ).astype(bf)

    grad_mat_proj_t = both(grad_lows, hiddens, (0, 1), (0, 1))
    grad_mat_fc = both(own_columns(seconds), grad_ins, (0, 1), (0, 1))
    grad_mat_out = both(attendeds, branches, (0, 2), (0, 1))

    grad_sent, grad_sent_last = attend_grad(
        got, got_last, limit, unit_places, out_f, lse, grad_got, grad_got_last
    )
    back, back_last = exchange(5, -1, grad_sent, grad_sent_last)
    last_parts = back[:, 192:256, :].astype(f32).reshape(2, half, HEAD_DIM, 256)
    last_sums = jnp.sum(last_parts, 1).astype(bf)
    grad_query = jnp.concatenate(
        [back[:, 0:64].reshape(cut, count), jnp.concatenate([back_last[0], back_last[1]], 1)], 0
    )
    grad_key = jnp.concatenate(
        [
            back[:, 64:128].reshape(cut, count),
            jnp.concatenate([last_sums[0, :, :128], last_sums[1, :, :128]], 1),
        ],
        0,
    )
    grad_value = jnp.concatenate(
        [
            back[:, 128:192].reshape(cut, count),
            jnp.concatenate([last_sums[0, :, 128:], last_sums[1, :, 128:]], 1),
        ],
        0,
    )
    grad_bias_query = jnp.sum(grad_query, 1, dtype=f32).reshape(1, width)
    grad_bias_value = jnp.sum(grad_value, 1, dtype=f32).reshape(1, width)
    grad_joined = jnp.concatenate([grad_query, grad_key, grad_value], 0)
    (joined_pair,) = share(6, grad_joined)
    grad_mat_qkv = both(own_columns(firsts), joined_pair, (0, 1), (0, 2))
    grad_first = contract(grad_joined, mat_qkv, 0, 1)
    grad_rows_norm, grad_gain_one, grad_shift_one = norm_back(
        grad_first, unit_one, spread_one, gain_one
    )
    tokens_grad = (grad_middle + grad_rows_norm).astype(bf).reshape(micro, 1, rows_here, width)

    small_grads = jnp.concatenate(
        [
            grad_gain_one,
            grad_shift_one,
            grad_bias_query,
            grad_bias_value,
            grad_bias_out,
            grad_gain_two,
            grad_shift_two,
            grad_bias_proj,
            grad_bias_fc.reshape(-1, width),
            jnp.zeros((4, width), f32),
        ],
        0,
    )
    sum_proj_t, sum_fc, sum_out, sum_qkv, small_sum = sum_grads(
        7,
        grad_mat_proj_t,
        grad_mat_fc,
        jnp.pad(grad_mat_out, ((0, 0), (0, 1280 - width))),
        jnp.pad(grad_mat_qkv, ((0, 0), (0, 3328 - 3 * width))),
        small_grads.reshape(2, 8, width),
    )
    own_rows = lax.dynamic_slice_in_dim(small_sum[0], group * part, part, 1)
    vec = [own_rows[i] for i in range(8)]
    bias_rows = lax.dynamic_slice_in_dim(small_sum[1], group * 2, 2, 0).reshape(-1)
    return (
        result,
        tokens_grad,
        vec[0],
        vec[1],
        sum_qkv[:, : 3 * width].astype(f32),
        vec[2],
        vec[3],
        sum_out[:, :width].astype(f32),
        vec[4],
        vec[5],
        vec[6],
        sum_fc.astype(f32),
        bias_rows,
        sum_proj_t.astype(f32).T,
        vec[7],
    )


def specs():
    wide = P(None, "group", "replica", None)
    row, mat = P("group"), P("group", None)
    in_specs = (wide, wide, P(None, "group", "replica"), P(None, "group"))
    in_specs += (row, row, mat, row, row, mat, row, row, row, mat, row, mat, row)
    out_specs = (wide, wide, row, row, mat, row, row, mat, row, row, row, mat, row, mat, row)
    return in_specs, out_specs


def solution(mesh):
    by_heads = mesh.shape["replica"] == HEADS - 1 and mesh.shape["group"] == 2
    in_specs, out_specs = specs()
    return jax.shard_map(
        per_device_heads if by_heads else per_device_gather,
        mesh=mesh,
        in_specs=in_specs,
        out_specs=out_specs,
        check_vma=False,
    )
```

```python
import functools

import jax
import jax.numpy as jnp
from jax import lax
from jax.experimental import pallas as pl
from jax.experimental.pallas import tpu as pltpu
from jax.sharding import PartitionSpec as P

HEADS = 17
HEAD_DIM = 64
MESH = pl.DeviceIdType.MESH


def for_sending(array):

    def short(part):
        return part.astype(jnp.bfloat16) if part.dtype == jnp.float32 else part

    return jax.tree.map(short, array)


def norm_rows(values, gain, shift):
    center = values - jnp.mean(values, -1, keepdims=True)
    spread = jnp.mean(center * center, -1, keepdims=True)
    return center * lax.rsqrt(spread + 1e-05) * gain + shift


def gelu_tanh(values):
    return jax.nn.gelu(values, approximate=True)


def inner_rows(left, right):
    return lax.dot_general(
        left, right, (((0,), (0,)), ((), ())), preferred_element_type=jnp.float32
    )


def times_transposed(left, right):
    return lax.dot_general(
        left, right, (((1,), (1,)), ((), ())), preferred_element_type=jnp.float32
    )


def masked_scores(queries, keys, query_place, key_place, prefix_len, scale):
    scores = jnp.einsum("qhe,khe->hqk", queries, keys, preferred_element_type=jnp.float32) * scale
    allowed = (key_place[None, :] <= query_place[:, None]) | (key_place[None, :] < prefix_len)
    return jnp.where(allowed[None], scores, -1e30)


def reduce_grads(terms):
    owned = jax.tree.map(
        lambda part: part.astype(jnp.float32),
        lax.psum_scatter(for_sending(terms), "group", scatter_dimension=0, tiled=True),
    )
    return jax.tree.map(
        lambda part: part.astype(jnp.float32), lax.psum(for_sending(owned), "replica")
    )


def per_device_gather(
    tokens,
    out_grad,
    positions,
    prefix,
    ln1_gain,
    ln1_bias,
    w_qkv,
    b_query,
    b_value,
    w_attn_out,
    b_attn_out,
    ln2_gain,
    ln2_bias,
    w_fc,
    b_fc,
    w_proj,
    b_proj,
):
    shards = (
        ln1_gain,
        ln1_bias,
        w_qkv,
        b_query,
        b_value,
        w_attn_out,
        b_attn_out,
        ln2_gain,
        ln2_bias,
        w_fc,
        b_fc,
        w_proj,
        b_proj,
    )
    micro = tokens.shape[0]
    rows_here = tokens.shape[2]
    width = tokens.shape[3]
    scale = HEAD_DIM ** (-0.5)
    head_shape = (rows_here, HEADS, HEAD_DIM)
    all_places = lax.all_gather(positions, "replica", axis=2, tiled=True)
    outputs_list = []
    grads_list = []
    kept = None
    owned = None
    for step in range(micro):
        full = (
            lax.all_gather(shards[0], "group", axis=0, tiled=True),
            lax.all_gather(shards[1], "group", axis=0, tiled=True),
            lax.all_gather(shards[2], "group", axis=0, tiled=True),
            lax.all_gather(shards[3], "group", axis=0, tiled=True),
            lax.all_gather(shards[4], "group", axis=0, tiled=True),
            lax.all_gather(shards[5], "group", axis=0, tiled=True),
            lax.all_gather(shards[6], "group", axis=0, tiled=True),
            lax.all_gather(shards[7], "group", axis=0, tiled=True),
            lax.all_gather(shards[8], "group", axis=0, tiled=True),
            lax.all_gather(shards[9], "group", axis=0, tiled=True),
            lax.all_gather(shards[10], "group", axis=0, tiled=True),
            lax.all_gather(shards[11], "group", axis=0, tiled=True),
            lax.all_gather(shards[12], "group", axis=0, tiled=True),
        )
        (
            gain_one,
            shift_one,
            mat_qkv,
            bias_query,
            bias_value,
            mat_out,
            bias_out,
            gain_two,
            shift_two,
            mat_fc,
            bias_fc,
            mat_proj,
            bias_proj,
        ) = full
        gain_one = gain_one.astype(jnp.float32)
        shift_one = shift_one.astype(jnp.float32)
        bias_query = bias_query.astype(jnp.float32)
        bias_value = bias_value.astype(jnp.float32)
        bias_out = bias_out.astype(jnp.float32)
        gain_two = gain_two.astype(jnp.float32)
        shift_two = shift_two.astype(jnp.float32)
        bias_fc = bias_fc.astype(jnp.float32)
        bias_proj = bias_proj.astype(jnp.float32)
        rows_in = tokens[step, 0].astype(jnp.float32)
        query_place = positions[step, 0]
        key_place = all_places[step, 0]
        prefix_len = prefix[step, 0]
        normed_one, norm_one_pull = jax.vjp(norm_rows, rows_in, gain_one, shift_one)
        first = normed_one.astype(jnp.bfloat16)
        joined = jnp.dot(first, mat_qkv, preferred_element_type=jnp.float32)
        queries = (joined[:, :width] + bias_query).astype(jnp.bfloat16)
        keys = joined[:, width : 2 * width].astype(jnp.bfloat16)
        values = (joined[:, 2 * width :] + bias_value).astype(jnp.bfloat16)
        key_all, value_all = (
            lax.all_gather(keys, "replica", axis=0, tiled=True),
            lax.all_gather(values, "replica", axis=0, tiled=True),
        )
        length = key_all.shape[0]
        block = min(512, length)
        nblocks = length // block
        query_heads = queries.reshape(head_shape)
        key_blocks = key_all.reshape(nblocks, block, HEADS, HEAD_DIM)
        value_blocks = value_all.reshape(nblocks, block, HEADS, HEAD_DIM)
        place_blocks = key_place.reshape(nblocks, block)

        def attend_step(carry, blockargs):
            highest, total, summed = carry
            key_part, value_part, place_part = blockargs
            scores = masked_scores(
                query_heads, key_part, query_place, place_part, prefix_len, scale
            )
            new_high = jnp.maximum(highest, jnp.max(scores, -1))
            factor = jnp.exp(highest - new_high)
            expo = jnp.exp(scores - new_high[..., None])
            total = total * factor + jnp.sum(expo, -1)
            summed = summed * jnp.transpose(factor)[..., None] + jnp.einsum(
                "hqk,khe->qhe",
                expo.astype(jnp.bfloat16),
                value_part,
                preferred_element_type=jnp.float32,
            )
            return ((new_high, total, summed), None)

        start_carry = (
            jnp.full((HEADS, rows_here), -1e30, jnp.float32),
            jnp.zeros((HEADS, rows_here), jnp.float32),
            jnp.zeros(head_shape, jnp.float32),
        )
        (highest, total, summed), _ = lax.scan(
            attend_step, start_carry, (key_blocks, value_blocks, place_blocks)
        )
        log_total = highest + jnp.log(total)
        attended_f = summed / jnp.transpose(total)[..., None]
        attended = attended_f.reshape(rows_here, width).astype(jnp.bfloat16)
        middle = rows_in + jnp.dot(attended, mat_out, preferred_element_type=jnp.float32) + bias_out
        normed_two, norm_two_pull = jax.vjp(norm_rows, middle, gain_two, shift_two)
        second = normed_two.astype(jnp.bfloat16)
        hidden_in = jnp.dot(second, mat_fc, preferred_element_type=jnp.float32) + bias_fc
        hidden_f, gelu_pull = jax.vjp(gelu_tanh, hidden_in)
        hidden = hidden_f.astype(jnp.bfloat16)
        output_rows = (
            middle + jnp.dot(hidden, mat_proj, preferred_element_type=jnp.float32) + bias_proj
        )
        outputs_list.append(output_rows.astype(jnp.bfloat16))
        grad_top = out_grad[step, 0].astype(jnp.float32)
        grad_low = out_grad[step, 0]
        grad_bias_proj = jnp.sum(grad_top, 0)
        grad_mat_proj = inner_rows(hidden, grad_low)
        grad_hidden = times_transposed(grad_low, mat_proj)
        (grad_hidden_in,) = gelu_pull(grad_hidden)
        grad_hidden_in = grad_hidden_in.astype(jnp.bfloat16)
        grad_bias_fc = jnp.sum(grad_hidden_in, 0, dtype=jnp.float32)
        grad_mat_fc = inner_rows(second, grad_hidden_in)
        grad_second = times_transposed(grad_hidden_in, mat_fc)
        grad_middle_norm, grad_gain_two, grad_shift_two = norm_two_pull(grad_second)
        grad_middle = grad_top + grad_middle_norm
        grad_bias_out = jnp.sum(grad_middle, 0)
        grad_branch = grad_middle.astype(jnp.bfloat16)
        grad_mat_out = inner_rows(attended, grad_branch)
        grad_attended = times_transposed(grad_branch, mat_out).astype(jnp.bfloat16)
        grad_heads = grad_attended.reshape(head_shape)
        delta = jnp.transpose(jnp.sum(grad_heads.astype(jnp.float32) * attended_f, -1))

        def score_grads(
            query_part, grad_part, key_part, value_part, qplace, kplace, lse_part, delta_part
        ):
            scores = masked_scores(query_part, key_part, qplace, kplace, prefix_len, scale)
            probs = jnp.exp(scores - lse_part[..., None])
            grad_probs = jnp.einsum(
                "qhe,khe->hqk", grad_part, value_part, preferred_element_type=jnp.float32
            )
            grad_scores = (probs * (grad_probs - delta_part[..., None])).astype(jnp.bfloat16)
            return (probs.astype(jnp.bfloat16), grad_scores)

        def grad_step(summed, blockargs):
            key_part, value_part, place_part = blockargs
            probs, grad_scores = score_grads(
                query_heads,
                grad_heads,
                key_part,
                value_part,
                query_place,
                place_part,
                log_total,
                delta,
            )
            summed = summed + jnp.einsum(
                "hqk,khe->qhe", grad_scores, key_part, preferred_element_type=jnp.float32
            )
            key_grad = jnp.einsum(
                "hqk,qhe->khe", grad_scores, query_heads, preferred_element_type=jnp.float32
            )
            value_grad = jnp.einsum(
                "hqk,qhe->khe", probs, grad_heads, preferred_element_type=jnp.float32
            )
            return (summed, (key_grad, value_grad))

        grad_query, (key_grads, value_grads) = lax.scan(
            grad_step, jnp.zeros(head_shape, jnp.float32), (key_blocks, value_blocks, place_blocks)
        )
        grad_key, grad_value = (
            lax.psum_scatter(
                key_grads.reshape(length, width).astype(jnp.bfloat16),
                "replica",
                scatter_dimension=0,
                tiled=True,
            ).astype(jnp.float32),
            lax.psum_scatter(
                value_grads.reshape(length, width).astype(jnp.bfloat16),
                "replica",
                scatter_dimension=0,
                tiled=True,
            ).astype(jnp.float32),
        )
        grad_query = (grad_query.reshape(rows_here, width) * scale).astype(jnp.bfloat16)
        grad_key = (grad_key * scale).astype(jnp.bfloat16)
        grad_value = grad_value.astype(jnp.bfloat16)
        grad_bias_query = jnp.sum(grad_query, 0, dtype=jnp.float32)
        grad_bias_value = jnp.sum(grad_value, 0, dtype=jnp.float32)
        grad_joined = jnp.concatenate([grad_query, grad_key, grad_value], 1)
        grad_mat_qkv = inner_rows(first, grad_joined)
        grad_first = times_transposed(grad_joined, mat_qkv)
        grad_rows_norm, grad_gain_one, grad_shift_one = norm_one_pull(grad_first)
        grads_list.append((grad_middle + grad_rows_norm).astype(jnp.bfloat16))
        terms = (
            grad_gain_one,
            grad_shift_one,
            grad_mat_qkv,
            grad_bias_query,
            grad_bias_value,
            grad_mat_out,
            grad_bias_out,
            grad_gain_two,
            grad_shift_two,
            grad_mat_fc,
            grad_bias_fc,
            grad_mat_proj,
            grad_bias_proj,
        )
        kept = (
            terms
            if kept is None
            else tuple((first_term + second_term for first_term, second_term in zip(kept, terms)))
        )
    owned = reduce_grads(kept)
    result = jnp.stack(outputs_list).reshape(micro, 1, rows_here, width)
    tokens_grad = jnp.stack(grads_list).reshape(micro, 1, rows_here, width)
    return (result, tokens_grad) + tuple(owned)


def contract(left, right, left_dim, right_dim):
    return lax.dot_general(
        left, right, (((left_dim,), (right_dim,)), ((), ())), preferred_element_type=jnp.float32
    )


def greet(peers, here, group_too):
    barrier = pltpu.get_barrier_semaphore()

    def one(step, carry):
        peer = lax.rem(here + step, peers)
        pl.semaphore_signal(barrier, inc=1, device_id={"replica": peer}, device_id_type=MESH)
        return carry

    lax.fori_loop(1, peers, one, 0)
    if group_too:
        other = 1 - lax.axis_index("group")
        pl.semaphore_signal(barrier, inc=1, device_id={"group": other}, device_id_type=MESH)
    pl.semaphore_wait(barrier, peers - 1 + (1 if group_too else 0))


def halves(ref, mode, which):
    if mode == "whole":
        return ref
    if mode == "rows":
        size = ref.shape[0] // 2
        return ref.at[pl.ds(pl.multiple_of(which * size, 16), size)]
    size = ref.shape[1] // 2
    return ref.at[:, pl.ds(pl.multiple_of(which * size, 128), size)]


def half_shape(array, mode):
    rows, columns = array.shape
    return {"whole": (rows, columns), "rows": (rows // 2, columns), "columns": (rows, columns // 2)}[mode]


def exchange_body(direction, with_places, modes, *refs):
    refs = list(refs)
    nweights = len(modes)
    chunk, last = refs.pop(0), refs.pop(0)
    places = refs.pop(0) if with_places else None
    weights = [refs.pop(0) for _ in range(nweights)]
    chunk_out, last_out = refs.pop(0), refs.pop(0)
    places_out = refs.pop(0) if with_places else None
    weights_out = [refs.pop(0) for _ in range(nweights)]
    send, recv, last_send, last_recv, own = (refs.pop(0) for _ in range(5))
    if with_places:
        place_send, place_recv = refs.pop(0), refs.pop(0)
    if nweights:
        weight_send, weight_recv, weight_own = (refs.pop(0) for _ in range(3))
        bounce = [refs.pop(0) for _ in range(nweights)]
    peers = chunk.shape[0]
    here = lax.axis_index("replica")
    group = lax.axis_index("group")
    greet(peers, here, nweights > 0)
    loads, copies = [], []
    for i in range(nweights):
        copy = pltpu.make_async_remote_copy(
            halves(weights[i], modes[i], 1 - group),
            weights_out[i].at[group],
            weight_send.at[i],
            weight_recv.at[i],
            device_id={"group": 1 - group},
            device_id_type=MESH,
        )
        copy.start()
        copies.append(copy)
        load = pltpu.make_async_copy(
            halves(weights[i], modes[i], group), bounce[i], weight_own.at[i]
        )
        load.start()
        loads.append(load)
    for slot in range(2):
        half = peers // 2
        target = lax.rem(here + direction + peers, half) + half * slot
        copy = pltpu.make_async_remote_copy(
            last.at[slot],
            last_out.at[here // half],
            last_send.at[slot],
            last_recv.at[here // half],
            device_id={"replica": target},
            device_id_type=MESH,
        )
        copy.start()
        copies.append(
            (
                copy,
                pltpu.make_async_remote_copy(
                    last.at[slot],
                    last_out.at[slot],
                    last_send.at[slot],
                    last_recv.at[slot],
                    device_id={"replica": target},
                    device_id_type=MESH,
                ),
            )
        )
    for step in range(1, peers):
        peer = lax.rem(here + step, peers)
        copy = pltpu.make_async_remote_copy(
            chunk.at[peer],
            chunk_out.at[here],
            send.at[step],
            recv.at[step],
            device_id={"replica": peer},
            device_id_type=MESH,
        )
        copy.start()
        copies.append(copy)
        if with_places:
            copy = pltpu.make_async_remote_copy(
                places,
                places_out.at[here],
                place_send.at[step],
                place_recv.at[step],
                device_id={"replica": peer},
                device_id_type=MESH,
            )
            copy.start()
            copies.append(copy)
    owns = [pltpu.make_async_copy(chunk.at[here], chunk_out.at[here], own.at[0])]
    if with_places:
        owns.append(pltpu.make_async_copy(places, places_out.at[here], own.at[1]))
    for copy in owns:
        copy.start()
    stores = []
    for i, load in enumerate(loads):
        load.wait()
        store = pltpu.make_async_copy(bounce[i], weights_out[i].at[group], weight_own.at[i])
        store.start()
        stores.append(store)
    for copy in stores + owns:
        copy.wait()
    for copy in copies:
        if isinstance(copy, tuple):
            copy[0].wait_send()
            copy[1].wait_recv()
        else:
            copy.wait()


def exchange(ident, direction, chunk, last, places=None, shares=()):
    peers = chunk.shape[0]
    weights = [array for array, _ in shares]
    modes = [mode for _, mode in shares]
    any_spec = pl.BlockSpec(memory_space=pl.ANY)
    with_places = places is not None
    args = [chunk, last] + ([places] if with_places else []) + list(weights)
    shapes = [(chunk.shape, chunk.dtype), (last.shape, last.dtype)]
    if with_places:
        shapes.append(((peers,) + places.shape, places.dtype))
    shapes += [((2,) + half_shape(*item), item[0].dtype) for item in shares]
    dma = pltpu.SemaphoreType.DMA
    scratch = [dma((peers,)), dma((peers,)), dma((2,)), dma((2,)), dma((2,))]
    if with_places:
        scratch += [dma((peers,)), dma((peers,))]
    if weights:
        count = len(weights)
        scratch += [dma((count,)), dma((count,)), dma((count,))]
        scratch += [pltpu.VMEM(half_shape(*item), item[0].dtype) for item in shares]
    return pl.pallas_call(
        functools.partial(exchange_body, direction, with_places, modes),
        out_shape=[jax.ShapeDtypeStruct(*shape) for shape in shapes],
        in_specs=[any_spec] * len(args),
        out_specs=[any_spec] * len(shapes),
        scratch_shapes=scratch,
        compiler_params=pltpu.CompilerParams(collective_id=ident, has_side_effects=True),
        name=f"exchange{ident}",
    )(*args)


def share_body(count, *refs):
    sources, results = refs[:count], refs[count : 2 * count]
    send, recv, own = refs[2 * count : 2 * count + 3]
    bounce = refs[2 * count + 3 :]
    group = lax.axis_index("group")
    barrier = pltpu.get_barrier_semaphore()
    pl.semaphore_signal(barrier, inc=1, device_id={"group": 1 - group}, device_id_type=MESH)
    pl.semaphore_wait(barrier, 1)
    copies, loads, stores = [], [], []
    for i in range(count):
        copy = pltpu.make_async_remote_copy(
            sources[i],
            results[i].at[group],
            send.at[i],
            recv.at[i],
            device_id={"group": 1 - group},
            device_id_type=MESH,
        )
        copy.start()
        copies.append(copy)
        load = pltpu.make_async_copy(sources[i], bounce[i], own.at[i])
        load.start()
        loads.append(load)
    for i in range(count):
        loads[i].wait()
        store = pltpu.make_async_copy(bounce[i], results[i].at[group], own.at[i])
        store.start()
        stores.append(store)
    for copy in stores + copies:
        copy.wait()


def share(ident, *arrays):
    count = len(arrays)
    any_spec = pl.BlockSpec(memory_space=pl.ANY)
    dma = pltpu.SemaphoreType.DMA
    return pl.pallas_call(
        functools.partial(share_body, count),
        out_shape=[jax.ShapeDtypeStruct((2,) + a.shape, a.dtype) for a in arrays],
        in_specs=[any_spec] * count,
        out_specs=[any_spec] * count,
        scratch_shapes=[dma((count,)), dma((count,)), dma((count,))]
        + [pltpu.VMEM(a.shape, a.dtype) for a in arrays],
        compiler_params=pltpu.CompilerParams(collective_id=ident, has_side_effects=True),
        name=f"share{ident}",
    )(*arrays)


BLOCK = 256


def unpack_units(got, last, rows_at, query_out):
    peers = got.shape[0]
    half = BLOCK // 128
    for m in range(2):
        for s in range(peers):
            query_out[m * (peers // half) + s // half, :, (s % half) * 128 : (s % half + 1) * 128] = got[
                s, rows_at : rows_at + 64, m * 128 : (m + 1) * 128
            ]
    extra = 2 * (peers // half)
    for j in range(2):
        query_out[extra, :, j * 128 : (j + 1) * 128] = last[j]


def unit_source(got, u, s, first):
    if u < 2:
        return got[s, first : first + 64, u * 128 : (u + 1) * 128]
    at = 0 if first == 64 else 128
    return got[s, 192:256, at : at + 128]


def attend_body(got, last, limit, places, sent, last_sent, out_f, lse, keys, values, queries, outs):
    peers = got.shape[0]
    nblocks = queries.shape[0]
    per_unit = (nblocks - 1) // 2
    unpack_units(got, last, 0, queries)
    for u in range(3):
        for s in range(peers):
            span = slice(s * 128, (s + 1) * 128)
            keys[u, span, :] = unit_source(got, u, s, 64).T
            values[u, :, span] = unit_source(got, u, s, 128)

    def block(b, carry):
        u = b // per_unit
        scores = jnp.dot(keys[u], queries[b], preferred_element_type=jnp.float32)
        place = places[jnp.where(u == 2, lax.axis_index("replica") // (peers // 2), u)]
        place = jnp.concatenate([place, place], axis=1)
        scores = jnp.where(place < limit[b], scores, -1e30)
        high = jnp.max(scores, axis=0, keepdims=True)
        expo = jnp.exp(scores - high)
        total = jnp.sum(expo, axis=0, keepdims=True)
        summed = jnp.dot(values[u], expo.astype(jnp.bfloat16), preferred_element_type=jnp.float32)
        result = summed / total
        out_f[b] = result
        outs[b] = result.astype(jnp.bfloat16)
        lse[b] = high + jnp.log(total)
        return carry

    lax.fori_loop(0, nblocks, block, 0)
    half = BLOCK // 128
    for m in range(2):
        for s in range(peers):
            sent[s, :, m * 128 : (m + 1) * 128] = outs[
                m * per_unit + s // half, :, (s % half) * 128 : (s % half + 1) * 128
            ]
    for j in range(2):
        last_sent[j] = outs[nblocks - 1, :, j * 128 : (j + 1) * 128]


def attend(got, last, limit, places):
    peers = got.shape[0]
    nblocks = limit.shape[0]
    length = places.shape[1]
    bf, f32 = jnp.bfloat16, jnp.float32
    return pl.pallas_call(
        attend_body,
        out_shape=[
            jax.ShapeDtypeStruct((peers, 64, 256), bf),
            jax.ShapeDtypeStruct((2, 64, 128), bf),
            jax.ShapeDtypeStruct((nblocks, 64, BLOCK), f32),
            jax.ShapeDtypeStruct((nblocks, 1, BLOCK), f32),
        ],
        scratch_shapes=[
            pltpu.VMEM((3, length, 64), bf),
            pltpu.VMEM((3, 64, length), bf),
            pltpu.VMEM((nblocks, 64, BLOCK), bf),
            pltpu.VMEM((nblocks, 64, BLOCK), bf),
        ],
        compiler_params=pltpu.CompilerParams(vmem_limit_bytes=56 << 20),
        name="attend",
    )(got, last, limit, places)


ROWS = 272
PART = 80
PADDED = 4 * PART
PROJ, FC, OUT, QKV = range(4)
TILES = {PROJ: (9, 8), FC: (9, 8), OUT: (5,), QKV: (7, 6)}


def chunk_plan():
    plan = []
    for array in (PROJ, FC, OUT, QKV):
        start = 0
        for tiles in TILES[array]:
            plan.append((array, tiles * 128, start))
            start += tiles * 128
    return plan


def piece(ref, item, first, second):
    array, width, start = item
    if array == PROJ:
        row = first * (2 * ROWS) + second * ROWS
        return ref.at[pl.ds(pl.multiple_of(row, 16), ROWS), pl.ds(start, width)]
    column = second * (sum(TILES[array]) * 128) + start
    return ref.at[
        pl.ds(pl.multiple_of(first * ROWS, 16), ROWS), pl.ds(pl.multiple_of(column, 128), width)
    ]


def by_rows(rows, fn):
    def one(i, carry):
        fn(pl.multiple_of(i * 16, 16))
        return carry

    lax.fori_loop(0, rows // 16, one, 0)


class Summer:
    def __init__(self, plan, sources, results, own, came, second_in, parts, summed, gathered, sems):
        self.plan, self.sources, self.results = plan, sources, results
        self.own, self.came, self.second_in = own, came, second_in
        self.parts, self.summed, self.gathered = parts, summed, gathered
        self.load_sem, self.store_sem, self.keep_sem = sems[0], sems[1], sems[2]
        self.pairs = [tuple(sems[3 + 2 * i : 5 + 2 * i]) for i in range(6)]
        here, group = lax.axis_index("replica"), lax.axis_index("group")
        bit_x, bit_y = here % 2, (here // 2) % 2
        self.here, self.place = here, here // 4
        self.one = bit_x + group * (bit_y - bit_x)
        self.two = bit_x + bit_y - self.one
        self.peer_one = here + (1 + group) * (1 - 2 * self.one)
        self.peer_two = here + (2 - group) * (1 - 2 * self.two)

    def copy(self, stage, at, source, target, peer):
        send, recv = self.pairs[stage]
        return pltpu.make_async_remote_copy(
            source,
            target,
            send.at[at],
            recv.at[at],
            device_id={"replica": peer},
            device_id_type=MESH,
        )

    def z_peer(self, k):
        return lax.rem(self.here + 4 * k, 16)

    def block(self, place):
        return pl.ds(pl.multiple_of(place * PART, 16), PART)

    def load(self, c, j):
        item = self.plan[c]
        source = piece(self.sources[item[0]], item, self.one, j)
        target = self.own[c].at[j, pl.ds(0, ROWS)]
        return pltpu.make_async_copy(source, target, self.load_sem.at[c, j])

    def first(self, c, j):
        item = self.plan[c]
        source = piece(self.sources[item[0]], item, 1 - self.one, j)
        return self.copy(0, (c, j), source, self.came[c].at[j], self.peer_one)

    def second(self, c):
        source = self.own[c].at[1 - self.two, pl.ds(0, ROWS)]
        return self.copy(1, (c,), source, self.second_in[c], self.peer_two)

    def spread(self, c, k):
        source = self.own[c].at[self.two, self.block(lax.rem(self.place + k, 4))]
        return self.copy(2, (c, k - 1), source, self.parts[c].at[k - 1], self.z_peer(k))

    def gather(self, c, k):
        target = self.gathered[c].at[self.block(self.place)]
        return self.copy(3, (c, k - 1), self.summed[c], target, self.z_peer(k))

    def keep(self, c):
        target = self.gathered[c].at[self.block(self.place)]
        return pltpu.make_async_copy(self.summed[c], target, self.keep_sem.at[c])

    def result(self, c, other):
        item = self.plan[c]
        second = self.two + other * (1 - 2 * self.two)
        return piece(self.results[item[0]], item, self.one, second)

    def cross(self, c):
        return self.copy(
            4, (c,), self.gathered[c].at[pl.ds(0, ROWS)], self.result(c, 0), self.peer_two
        )

    def crossed(self, c):
        return self.copy(
            4, (c,), self.gathered[c].at[pl.ds(0, ROWS)], self.result(c, 1), self.peer_two
        )

    def final(self, c, other):
        source = self.result(c, 1) if other else self.gathered[c].at[pl.ds(0, ROWS)]
        return self.copy(5, (c, other), source, self.result(c, other), self.peer_one)

    def finalled(self, c, other):
        item = self.plan[c]
        second = self.two + other * (1 - 2 * self.two)
        target = piece(self.results[item[0]], item, 1 - self.one, second)
        source = self.result(c, 1) if other else self.gathered[c].at[pl.ds(0, ROWS)]
        return self.copy(5, (c, other), source, target, self.peer_one)

    def fetch(self, c):
        target = self.came[c].at[self.two]
        return pltpu.make_async_copy(
            self.gathered[c].at[pl.ds(0, ROWS)], target, self.store_sem.at[c]
        )

    def store(self, c):
        return pltpu.make_async_copy(
            self.came[c].at[self.two], self.result(c, 0), self.store_sem.at[c]
        )

    def begin(self, c):
        for j in range(2):
            self.first(c, j).start()
            self.load(c, j).start()
        width = self.own[c].shape[2]
        self.own[c][self.two, ROWS:, :] = jnp.zeros((PADDED - ROWS, width), jnp.bfloat16)

    def stage_one(self, c):
        for j in range(2):
            self.load(c, j).wait()
            self.first(c, j).wait_recv()
        away, own, came = 1 - self.two, self.own[c], self.came[c]

        def add(start):
            rows = pl.ds(start, 16)
            total = own[away, rows].astype(jnp.float32) + came[away, rows].astype(jnp.float32)
            own[away, rows] = total.astype(jnp.bfloat16)

        by_rows(ROWS, add)
        self.second(c).start()

    def stage_two(self, c):
        self.second(c).wait_recv()
        keep, own, came = self.two, self.own[c], self.came[c]

        def add(start):
            rows = pl.ds(start, 16)
            total = own[keep, rows].astype(jnp.float32) + came[keep, rows].astype(jnp.float32)
            total = total + self.second_in[c][rows].astype(jnp.float32)
            own[keep, rows] = total.astype(jnp.bfloat16)

        by_rows(ROWS, add)
        for k in (1, 2, 3):
            self.spread(c, k).start()

    def stage_three(self, c):
        for k in (1, 2, 3):
            self.spread(c, k).wait_recv()

        def add(start):
            at = pl.ds(pl.multiple_of(self.place * PART + start, 16), 16)
            total = self.own[c][self.two, at].astype(jnp.float32)
            for k in range(3):
                total = total + self.parts[c][k, pl.ds(start, 16)].astype(jnp.float32)
            self.summed[c][pl.ds(start, 16)] = total.astype(jnp.bfloat16)

        by_rows(PART, add)
        for k in (1, 2, 3):
            self.gather(c, k).start()
        self.keep(c).start()

    def stage_four(self, c):
        for k in (1, 2, 3):
            self.spread(c, k).wait_send()
            self.gather(c, k).wait_recv()
        self.keep(c).wait()
        self.cross(c).start()
        self.final(c, 0).start()
        self.fetch(c).start()

    def stage_five(self, c):
        self.crossed(c).wait_recv()
        self.final(c, 1).start()
        self.fetch(c).wait()
        self.store(c).start()

    def end(self, c):
        for j in range(2):
            self.finalled(c, j).wait_recv()
            self.first(c, j).wait_send()
            self.final(c, j).wait_send()
        self.second(c).wait_send()
        for k in (1, 2, 3):
            self.gather(c, k).wait_send()
        self.cross(c).wait_send()
        self.store(c).wait()

    def run(self, stage, c):
        steps = (self.stage_one, self.stage_two, self.stage_three, self.stage_four, self.stage_five)
        steps[stage](c)


def wavefront(chunks):
    order = []
    for tick in range(len(chunks) + 4):
        for stage in reversed(range(5)):
            if 0 <= tick - stage < len(chunks):
                order.append((stage, chunks[tick - stage]))
    return order


class SmallSum:
    def __init__(self, source, result, from_core, own, everyone, sems):
        self.source, self.result, self.from_core = source, result, from_core
        self.own, self.everyone = own, everyone
        (self.sp, self.rp, self.sa, self.ra, self.sb, self.rb) = sems
        self.here, self.group = lax.axis_index("replica"), lax.axis_index("group")
        self.peers = everyone.shape[0]

    def core_copy(self, source, target, send, recv):
        return pltpu.make_async_remote_copy(
            source,
            target,
            send,
            recv,
            device_id={"group": 1 - self.group},
            device_id_type=MESH,
        )

    def give(self):
        return self.core_copy(self.source.at[1 - self.group], self.from_core, self.sp, self.rp)

    def tell(self, step):
        return pltpu.make_async_remote_copy(
            self.own,
            self.everyone.at[self.here],
            self.sa.at[step],
            self.ra.at[step],
            device_id={"replica": lax.rem(self.here + step, self.peers)},
            device_id_type=MESH,
        )

    def back(self):
        return self.core_copy(
            self.result.at[self.group], self.result.at[self.group], self.sb, self.rb
        )

    def begin(self):
        self.give().start()

    def middle(self):
        self.give().wait()
        self.own[...] = self.source[self.group] + self.from_core[...]
        self.everyone[self.here] = self.own[...]
        for step in range(1, self.peers):
            self.tell(step).start()

    def finish(self):
        for step in range(1, self.peers):
            self.tell(step).wait()
        total = self.everyone[0]
        for i in range(1, self.peers):
            total = total + self.everyone[i]
        self.result[self.group] = total
        self.back().start()

    def end(self):
        self.back().wait()


def sum_buffers(plan):
    bf = jnp.bfloat16
    shapes = ((2, PADDED), (2, ROWS), (ROWS,), (3, PART), (PART,))
    return [pltpu.VMEM(shape + (item[1],), bf) for shape in shapes for item in plan]


def sum_sems(plan):
    dma = pltpu.SemaphoreType.DMA
    count = len(plan)
    pairs, triples, ones = dma((count, 2)), dma((count, 3)), dma((count,))
    stages = (pairs, ones, triples, triples, ones, pairs)
    return [pairs, ones, ones] + [sem for stage in stages for sem in (stage, stage)]


def small_scratch(shape, peers):
    f32 = jnp.float32
    return [pltpu.VMEM(shape, f32), pltpu.VMEM(shape, f32), pltpu.VMEM((peers,) + shape, f32)]


def small_sems(peers):
    dma = pltpu.SemaphoreType.DMA
    return [dma, dma, dma((peers,)), dma((peers,)), dma, dma]


def small_body(small, result, from_core, own, everyone, *sems):
    smalls = SmallSum(small, result, from_core, own, everyone, sems)
    greet(everyone.shape[0], lax.axis_index("replica"), True)
    smalls.begin()
    smalls.middle()
    smalls.finish()
    smalls.end()


def sum_small(ident, small):
    peers = lax.axis_size("replica")
    vmem = pl.BlockSpec(memory_space=pltpu.VMEM)
    return pl.pallas_call(
        small_body,
        out_shape=jax.ShapeDtypeStruct(small.shape, small.dtype),
        in_specs=[vmem],
        out_specs=vmem,
        scratch_shapes=small_scratch(small.shape[1:], peers) + small_sems(peers),
        compiler_params=pltpu.CompilerParams(collective_id=ident, has_side_effects=True),
        name=f"small{ident}",
    )(small)


JOINED = 3328


def backward_body(plan, *refs):
    refs = list(refs)
    nchunks = len(plan)
    got, last, limit, places, out_f, lse, grad_got, grad_last, firsts = (
        refs.pop(0) for _ in range(9)
    )
    sources = [refs.pop(0) for _ in range(3)]
    results = [refs.pop(0) for _ in range(4)]
    joined_out = refs.pop(0)
    gathered = [refs.pop(0) for _ in range(nchunks)]
    buffers = [[refs.pop(0) for _ in range(nchunks)] for _ in range(5)]
    (
        keys,
        keys_t,
        values,
        queries,
        grads,
        queries_n,
        grads_n,
        dqs,
        dk,
        dv,
        sent,
        back,
        last_sent,
        back_last,
        joined,
        rest,
    ) = (refs.pop(0) for _ in range(16))
    back_send, back_recv, last_send, last_recv, joined_send, joined_recv, joined_own = (
        refs.pop(0) for _ in range(7)
    )
    summer = Summer(plan, sources + [rest], results, *buffers, gathered, refs)
    here, group = lax.axis_index("replica"), lax.axis_index("group")
    peers = got.shape[0]
    half_peers = peers // 2
    nblocks = queries.shape[0]
    per_unit = (nblocks - 1) // 2
    half = BLOCK // 128
    scale = HEAD_DIM ** (-0.5)
    greet(peers, here, True)
    summer.begin(0)
    summer.begin(1)

    kinds = (
        (pl.ds(192, 64), pl.ds(0, 256)),
        (pl.ds(0, 192), pl.ds(0, 128)),
        (pl.ds(0, 192), pl.ds(128, 128)),
    )

    def back_copy(kind, step):
        peer = lax.rem(here + step, peers)
        rows, columns = kinds[kind]
        return pltpu.make_async_remote_copy(
            sent.at[peer, rows, columns],
            back.at[here, rows, columns],
            back_send.at[kind, step],
            back_recv.at[kind, step],
            device_id={"replica": peer},
            device_id_type=MESH,
        )

    def last_copy(slot, target_slot):
        target = lax.rem(here - 1 + peers, half_peers) + half_peers * slot
        return pltpu.make_async_remote_copy(
            last_sent.at[slot],
            back_last.at[target_slot],
            last_send.at[slot],
            last_recv.at[target_slot],
            device_id={"replica": target},
            device_id_type=MESH,
        )

    unpack_units(got, last, 0, queries)
    unpack_units(grad_got, grad_last, 0, grads)
    for u in range(3):
        for s in range(peers):
            span = slice(s * 128, (s + 1) * 128)
            part = unit_source(got, u, s, 64)
            keys[u, span, :] = part.T
            keys_t[u, :, span] = part
            values[u, span, :] = unit_source(got, u, s, 128).T

    def natural(b, carry):
        queries_n[b] = queries[b].T
        grads_n[b] = grads[b].T
        return carry

    lax.fori_loop(0, nblocks, natural, 0)

    def clear():
        dk[...] = jnp.zeros_like(dk)
        dv[...] = jnp.zeros_like(dv)

    def finish_last():
        for s in range(peers):
            span = slice(s * 128, (s + 1) * 128)
            sent[s, 192:256, 0:128] = dk[span, :].T.astype(jnp.bfloat16)
            sent[s, 192:256, 128:256] = dv[span, :].T.astype(jnp.bfloat16)
        for j in range(2):
            last_sent[j] = (dqs[nblocks - 1, :, j * 128 : (j + 1) * 128] * scale).astype(
                jnp.bfloat16
            )
        for slot in range(2):
            last_copy(slot, here // half_peers).start()
        for step in range(1, peers):
            back_copy(0, step).start()
        clear()

    def finish_unit(m):
        at = slice(m * 128, (m + 1) * 128)
        for s in range(peers):
            span = slice(s * 128, (s + 1) * 128)
            dq = dqs[m * per_unit + s // half, :, (s % half) * 128 : (s % half + 1) * 128]
            sent[s, 0:64, at] = (dq * scale).astype(jnp.bfloat16)
            sent[s, 64:128, at] = dk[span, :].T.astype(jnp.bfloat16)
            sent[s, 128:192, at] = dv[span, :].T.astype(jnp.bfloat16)
        for step in range(1, peers):
            back_copy(1 + m, step).start()
        clear()

    def block(i, carry):
        is_last = i == 0
        b = jnp.where(is_last, nblocks - 1, i - 1)
        u = jnp.where(is_last, 2, (i - 1) // per_unit)
        grad = grads[b]
        delta = jnp.sum(grad.astype(jnp.float32) * out_f[b], axis=0, keepdims=True)
        scores = jnp.dot(keys[u], queries[b], preferred_element_type=jnp.float32)
        place = places[jnp.where(is_last, here // half_peers, u)]
        place = jnp.concatenate([place, place], axis=1)
        scores = jnp.where(place < limit[b], scores, -1e30)
        probs = jnp.exp(scores - lse[b])
        grad_probs = jnp.dot(values[u], grad, preferred_element_type=jnp.float32)
        grad_scores = (probs * (grad_probs - delta)).astype(jnp.bfloat16)
        dqs[b] = jnp.dot(keys_t[u], grad_scores, preferred_element_type=jnp.float32)
        dk[...] += jnp.dot(grad_scores, queries_n[b], preferred_element_type=jnp.float32)
        dv[...] += jnp.dot(probs.astype(jnp.bfloat16), grads_n[b], preferred_element_type=jnp.float32)
        pl.when(is_last)(finish_last)

        @pl.when(i == per_unit - 1)
        def _():
            summer.stage_one(0)

        @pl.when(i == per_unit)
        def _():
            finish_unit(0)
            summer.begin(2)

        @pl.when(i == 2 * per_unit - 3)
        def _():
            summer.stage_one(1)
            summer.stage_two(0)

        return carry

    clear()
    lax.fori_loop(0, nblocks, block, 0)
    finish_unit(1)
    back[here] = sent[here]
    summer.begin(3)
    summer.begin(4)
    done = {(0, 0), (0, 1), (1, 0)}
    order = [step for step in wavefront(range(nchunks)) if step not in done]
    early = [(0, 2), (1, 1), (2, 0)]
    for step in early:
        summer.run(*step)
        order.remove(step)

    for slot in range(2):
        last_copy(slot, slot).wait_recv()
    for kind in range(3):
        for step in range(1, peers):
            back_copy(kind, step).wait_recv()
    for h in range(peers):
        for part in range(3):
            row = part * (HEADS * HEAD_DIM) + h * HEAD_DIM
            joined[group, row : row + HEAD_DIM, :] = back[h, part * 64 : part * 64 + 64, :]
    width = HEADS * HEAD_DIM
    tail = (HEADS - 1) * HEAD_DIM
    for m in range(2):
        at = slice(m * 128, (m + 1) * 128)
        joined[group, tail:width, at] = back_last[m]
        for part in (1, 2):
            columns = slice((part - 1) * 128, part * 128)
            total = back[m * half_peers, 192:256, columns].astype(jnp.float32)
            for i in range(1, half_peers):
                total = total + back[m * half_peers + i, 192:256, columns].astype(jnp.float32)
            row = part * width + tail
            joined[group, row : row + HEAD_DIM, at] = total.astype(jnp.bfloat16)
    joined[group, 3 * width :, :] = jnp.zeros((JOINED - 3 * width, 256), jnp.bfloat16)
    share_joined = pltpu.make_async_remote_copy(
        joined.at[group],
        joined.at[group],
        joined_send,
        joined_recv,
        device_id={"group": 1 - group},
        device_id_type=MESH,
    )
    share_joined.start()
    keep_joined = pltpu.make_async_copy(joined.at[group], joined_out, joined_own)
    keep_joined.start()
    for step in [(1, 2), (2, 1), (0, 3)]:
        summer.run(*step)
        order.remove(step)
    share_joined.wait_recv()

    def weights(n, carry):
        columns = pl.ds(pl.multiple_of(n * 256, 256), 256)
        total = jnp.zeros((firsts.shape[1], 256), jnp.float32)
        for core in range(2):
            total = total + lax.dot_general(
                firsts[core],
                joined[core, columns, :],
                (((1,), (1,)), ((), ())),
                preferred_element_type=jnp.float32,
            )
        rest[:, columns] = total.astype(jnp.bfloat16)
        return carry

    lax.fori_loop(0, JOINED // 256, weights, 0)
    summer.begin(5)
    summer.begin(6)
    for step in order:
        summer.run(*step)
    share_joined.wait_send()
    keep_joined.wait()
    for slot in range(2):
        last_copy(slot, slot).wait_send()
    for kind in range(3):
        for step in range(1, peers):
            back_copy(kind, step).wait_send()
    for c in range(nchunks):
        summer.end(c)


def backward(ident, attention, firsts, arrays):
    plan = chunk_plan()
    got, _, limit = attention[:3]
    peers, nblocks = got.shape[0], limit.shape[0]
    length = peers * 128
    bf, f32 = jnp.bfloat16, jnp.float32
    any_spec = pl.BlockSpec(memory_space=pl.ANY)
    vmem = pl.BlockSpec(memory_space=pltpu.VMEM)
    dma = pltpu.SemaphoreType.DMA
    rest_shape = (firsts.shape[1], JOINED)
    shapes = [a.shape for a in arrays] + [rest_shape, (JOINED, 256)]
    shapes += [(PADDED, item[1]) for item in plan]
    return pl.pallas_call(
        functools.partial(backward_body, plan),
        out_shape=[jax.ShapeDtypeStruct(shape, bf) for shape in shapes],
        in_specs=[vmem] * 9 + [any_spec] * 3,
        out_specs=[any_spec] * len(shapes),
        scratch_shapes=sum_buffers(plan)
        + [
            pltpu.VMEM((3, length, 64), bf),
            pltpu.VMEM((3, 64, length), bf),
            pltpu.VMEM((3, length, 64), bf),
            pltpu.VMEM((nblocks, 64, BLOCK), bf),
            pltpu.VMEM((nblocks, 64, BLOCK), bf),
            pltpu.VMEM((nblocks, BLOCK, 64), bf),
            pltpu.VMEM((nblocks, BLOCK, 64), bf),
            pltpu.VMEM((nblocks, 64, BLOCK), f32),
            pltpu.VMEM((length, 64), f32),
            pltpu.VMEM((length, 64), f32),
            pltpu.VMEM((peers, 256, 256), bf),
            pltpu.VMEM((peers, 256, 256), bf),
            pltpu.VMEM((2, 64, 128), bf),
            pltpu.VMEM((2, 64, 128), bf),
            pltpu.VMEM((2, JOINED, 256), bf),
            pltpu.VMEM(rest_shape, bf),
            dma((3, peers)),
            dma((3, peers)),
            dma((2,)),
            dma((2,)),
            dma,
            dma,
            dma,
        ]
        + sum_sems(plan),
        compiler_params=pltpu.CompilerParams(
            collective_id=ident, has_side_effects=True, vmem_limit_bytes=67043328
        ),
        name="backward",
    )(*attention, firsts, *arrays)


def norm_unit(values):
    center = values - jnp.mean(values, -1, keepdims=True)
    spread = lax.rsqrt(jnp.mean(center * center, -1, keepdims=True) + 1e-05)
    return center * spread, spread


def norm_back(grad, unit, spread, gain):
    grad_unit = grad * gain
    slope = jnp.mean(grad_unit * unit, -1, keepdims=True)
    back = spread * (grad_unit - jnp.mean(grad_unit, -1, keepdims=True) - unit * slope)
    return back, jnp.sum(grad * unit, 0, keepdims=True), jnp.sum(grad, 0, keepdims=True)


def split_last(array):
    return jnp.stack([array[:, :128], array[:, 128:]])


def per_device_heads(
    tokens,
    out_grad,
    positions,
    prefix,
    ln1_gain,
    ln1_bias,
    w_qkv,
    b_query,
    b_value,
    w_attn_out,
    b_attn_out,
    ln2_gain,
    ln2_bias,
    w_fc,
    b_fc,
    w_proj,
    b_proj,
):
    bf, f32 = jnp.bfloat16, jnp.float32
    micro, _, rows_here, width = tokens.shape
    peers = lax.axis_size("replica")
    hidden_width = 2 * b_fc.shape[0]
    half = peers // 2
    count = micro * rows_here
    here = lax.axis_index("replica")
    scale = HEAD_DIM ** (-0.5)
    split = (peers * HEAD_DIM, width)

    vectors = (ln1_gain, ln1_bias, b_query, b_value, b_attn_out, ln2_gain, ln2_bias, b_proj, b_fc)
    shared = share(1, w_qkv, *(vector.reshape(1, -1) for vector in vectors))
    mat_qkv = shared[0].reshape(width, 3 * width)
    part = width // 2
    (
        gain_one,
        shift_one,
        bias_query,
        bias_value,
        bias_out,
        gain_two,
        shift_two,
        bias_proj,
        bias_fc,
    ) = (vector.reshape(1, -1).astype(f32) for vector in shared[1:])

    rows_in = tokens.reshape(count, width).astype(f32)
    unit_one, spread_one = norm_unit(rows_in)
    first = (unit_one * gain_one + shift_one).astype(bf)
    joined = contract(mat_qkv, first, 0, 1)
    bias_all = jnp.concatenate([bias_query, jnp.zeros_like(bias_query), bias_value], 1)
    joined = joined + bias_all.reshape(-1, 1)
    queries = ((joined[:width]).astype(bf).astype(f32) * scale).astype(bf)
    keys = joined[width : 2 * width].astype(bf)
    values = joined[2 * width :].astype(bf)
    cut = split[0]
    main = [part_[:cut].reshape(peers, HEAD_DIM, count) for part_ in (queries, keys, values)]
    key_last, value_last = keys[cut:], values[cut:]
    tails = jnp.stack(
        [
            jnp.concatenate(
                [key_last[:, m * 128 : (m + 1) * 128], value_last[:, m * 128 : (m + 1) * 128]], 1
            )
            for m in range(2)
        ]
    )
    tails = jnp.repeat(tails, half, axis=0)
    chunk = jnp.concatenate(main + [tails], axis=1)
    grad_low = out_grad.reshape(count, width)
    got, got_last, all_places, mat_out, mat_fc, mat_proj_t, firsts, grad_lows = exchange(
        2,
        1,
        chunk,
        split_last(queries[cut:]),
        positions.reshape(micro, rows_here),
        [(item, "whole") for item in (w_attn_out, w_fc, w_proj.T)]
        + [(first.T, "rows"), (grad_low, "whole")],
    )
    mat_out = mat_out.reshape(width, width)
    mat_fc = mat_fc.reshape(width, hidden_width)

    place_rows = jnp.transpose(all_places, (1, 0, 2)).reshape(micro, peers * rows_here)
    limits = jnp.maximum(place_rows + 1, prefix.reshape(micro, 1))
    mine = here // half
    at = lax.rem(here - 1 + peers, half)
    own_limits = lax.dynamic_index_in_dim(limits, mine, 0, False).reshape(peers, rows_here)
    own_limits = jnp.concatenate(
        [
            lax.dynamic_index_in_dim(own_limits, at, 0, True),
            lax.dynamic_index_in_dim(own_limits, at + half, 0, True),
        ],
        1,
    )
    limit = jnp.concatenate([limits.reshape(-1, BLOCK), own_limits], 0)[:, None, :]
    key_places = jnp.broadcast_to(place_rows[:, :, None], place_rows.shape + (128,))

    sent, sent_last, out_f, lse = attend(got, got_last, limit, key_places)
    heads_out, heads_last = exchange(3, -1, sent, sent_last)
    attended = jnp.concatenate(
        [heads_out.reshape(cut, count), jnp.concatenate([heads_last[0], heads_last[1]], 1)], 0
    )

    middle = rows_in + contract(attended, mat_out, 0, 0) + bias_out
    unit_two, spread_two = norm_unit(middle)
    second = (unit_two * gain_two + shift_two).astype(bf)
    hidden_in = jnp.dot(second, mat_fc, preferred_element_type=f32) + bias_fc
    hidden_f, gelu_pull = jax.vjp(gelu_tanh, hidden_in)
    hidden = hidden_f.astype(bf)
    output_rows = middle + bias_proj
    half_hidden = hidden_width // 2
    for core in range(2):
        own_hidden = hidden[:, core * half_hidden : (core + 1) * half_hidden]
        output_rows = output_rows + contract(own_hidden, mat_proj_t[core], 1, 1)
    result = output_rows.astype(bf).reshape(micro, 1, rows_here, width)

    grad_top = grad_low.astype(f32)
    grad_bias_proj = jnp.sum(grad_top, 0, keepdims=True)
    grad_hidden = jnp.concatenate([contract(grad_low, mat_proj_t[core], 1, 0) for core in range(2)], 1)
    (grad_hidden_in,) = gelu_pull(grad_hidden)
    grad_hidden_in = grad_hidden_in.astype(bf)
    grad_bias_fc = jnp.sum(grad_hidden_in, 0, keepdims=True, dtype=f32)
    grad_second = times_transposed(grad_hidden_in, mat_fc)
    grad_middle_norm, grad_gain_two, grad_shift_two = norm_back(
        grad_second, unit_two, spread_two, gain_two
    )
    grad_middle = grad_top + grad_middle_norm
    grad_bias_out = jnp.sum(grad_middle, 0, keepdims=True)
    grad_branch = grad_middle.astype(bf)
    grad_attended = contract(mat_out, grad_branch, 1, 1).astype(bf)

    grad_got, grad_got_last, hiddens, seconds, grad_ins, attendeds, branches = exchange(
        4,
        1,
        grad_attended[:cut].reshape(peers, HEAD_DIM, count),
        split_last(grad_attended[cut:]),
        None,
        [
            (hidden, "columns"),
            (second, "whole"),
            (grad_hidden_in, "whole"),
            (attended, "rows"),
            (grad_branch, "whole"),
        ],
    )
    group = lax.axis_index("group")

    def own_columns(pair):
        return lax.dynamic_slice_in_dim(pair, group * part, part, 2)

    def both(left, right, left_dims, right_dims):
        return lax.dot_general(
            left, right, ((left_dims, right_dims), ((), ())), preferred_element_type=f32
        ).astype(bf)

    grad_mat_proj_t = both(grad_lows, hiddens, (0, 1), (0, 1))
    grad_mat_fc = both(own_columns(seconds), grad_ins, (0, 1), (0, 1))
    grad_mat_out = both(attendeds, branches, (0, 2), (0, 1))

    sums = backward(
        5,
        (got, got_last, limit, key_places, out_f, lse, grad_got, grad_got_last),
        firsts,
        (grad_mat_proj_t, grad_mat_fc, jnp.pad(grad_mat_out, ((0, 0), (0, 1280 - width)))),
    )
    sum_proj_t, sum_fc, sum_out, sum_qkv, grad_joined = sums[:5]
    grad_joined = grad_joined[: 3 * width]
    grad_bias_query = jnp.sum(grad_joined[:width], 1, dtype=f32).reshape(1, width)
    grad_bias_value = jnp.sum(grad_joined[2 * width :], 1, dtype=f32).reshape(1, width)
    grad_first = contract(grad_joined, mat_qkv, 0, 1)
    grad_rows_norm, grad_gain_one, grad_shift_one = norm_back(
        grad_first, unit_one, spread_one, gain_one
    )
    tokens_grad = (grad_middle + grad_rows_norm).astype(bf).reshape(micro, 1, rows_here, width)

    small_grads = jnp.concatenate(
        [
            grad_gain_one,
            grad_shift_one,
            grad_bias_query,
            grad_bias_value,
            grad_bias_out,
            grad_gain_two,
            grad_shift_two,
            grad_bias_proj,
            grad_bias_fc.reshape(-1, width),
            jnp.zeros((4, width), f32),
        ],
        0,
    )
    small_sum = sum_small(6, small_grads.reshape(2, 8, width))
    own_rows = lax.dynamic_slice_in_dim(small_sum[0], group * part, part, 1)
    vec = [own_rows[i] for i in range(8)]
    bias_rows = lax.dynamic_slice_in_dim(small_sum[1], group * 2, 2, 0).reshape(-1)
    return (
        result,
        tokens_grad,
        vec[0],
        vec[1],
        sum_qkv[:, : 3 * width].astype(f32),
        vec[2],
        vec[3],
        sum_out[:, :width].astype(f32),
        vec[4],
        vec[5],
        vec[6],
        sum_fc.astype(f32),
        bias_rows,
        sum_proj_t.astype(f32).T,
        vec[7],
    )


def specs():
    wide = P(None, "group", "replica", None)
    row, mat = P("group"), P("group", None)
    in_specs = (wide, wide, P(None, "group", "replica"), P(None, "group"))
    in_specs += (row, row, mat, row, row, mat, row, row, row, mat, row, mat, row)
    out_specs = (wide, wide, row, row, mat, row, row, mat, row, row, row, mat, row, mat, row)
    return in_specs, out_specs


def solution(mesh):
    by_heads = mesh.shape["replica"] == HEADS - 1 and mesh.shape["group"] == 2
    in_specs, out_specs = specs()
    return jax.shard_map(
        per_device_heads if by_heads else per_device_gather,
        mesh=mesh,
        in_specs=in_specs,
        out_specs=out_specs,
        check_vma=False,
    )
```
